32 devices in a mesh: data: 2 (over x), pp: 4 (over z), ep: 4 (over y, core).
Axes of the slice: x: 2, y: 2, z: 4, core: 2. Of those that a mesh axis runs over, the one named last changes fastest.
Arguments:
- expert_out: bfloat16 [8, 64, 320, 2048], P(('data', 'pp'), 'ep'), parts along dimension 0
- expert_ids: int32 [8, 4, 512, 8], P(('data', 'pp'), 'ep'), parts along dimension 0
- slot_ids: int32 [8, 4, 512, 8], P(('data', 'pp'), 'ep'), parts along dimension 0
- gate_vals: float32 [8, 4, 512, 8], P(('data', 'pp'), 'ep'), parts along dimension 0
- residual: bfloat16 [8, 4, 512, 2048], P(('data', 'pp'), 'ep'), parts along dimension 0
- norm_scale: float32 [4, 2048], P('pp')
- w_query: bfloat16 [4, 2048, 16, 128], P('pp')
- w_key: bfloat16 [4, 2048, 16, 128], P('pp')
- w_value: bfloat16 [4, 2048, 16, 128], P('pp')
- w_out: bfloat16 [4, 16, 128, 2048], P('pp')
Outputs:
- output: bfloat16 [8, 4, 512, 2048], P(('data', 'pp'), 'ep'), parts along dimension 0
There are 2 independent parts. The reference program is written for one: setup_inputs(seed, part) draws one part's arguments, and reference() takes and returns one part's arrays. A program takes and returns all parts, laid end to end along the dimension named above; an argument that names none is the same for every part.
All inputs are finite; a program needn't handle non-finite values.
Results may differ from the reference program's by a relative error of at most 0.02.
Values are sent between devices in bfloat16 or wider.
A program may use at most 1 GiB of HBM per device.

```python
import jax
import jax.numpy as jnp
from jax import lax

STAGES = 4
EP_DEVS = 4
SEQS_DEV = 1
SEQ_LEN = 512
D = 2048
HEADS = 16
HEAD = 128
EXPERTS = 64
TOP = 8
CAP_DEV = 80

NUM_SEQ = EP_DEVS * SEQS_DEV
TOKENS = NUM_SEQ * SEQ_LEN
TOK_DEV = SEQS_DEV * SEQ_LEN
CAPACITY = EP_DEVS * CAP_DEV
HIDDEN = HEADS * HEAD
NORM_EPS = 1e-6


def queue_pos(flat_ids):
    sort_order = jnp.argsort(flat_ids, stable=True)
    ordered = flat_ids[sort_order]
    first_pos = jnp.searchsorted(ordered, ordered, side='left')
    rank_sorted = jnp.arange(flat_ids.shape[0]) - first_pos
    return rank_sorted[jnp.argsort(sort_order, stable=True)]


def draw_routing(route_key):
    rank_key, noise_key = jax.random.split(route_key)
    rank_draw = jax.random.randint(rank_key, (STAGES, EXPERTS), 0, 1 << 20) * EXPERTS + jnp.arange(EXPERTS)
    expert_rank = jnp.argsort(rank_draw, axis=-1)
    hot_bias = jnp.where(expert_rank == 0, 4000, jnp.where(expert_rank < 3, 200, 0))
    stage_keys = jax.random.split(noise_key, STAGES)

    def pick_stage(stage_args):
        stage_key, stage_bias = stage_args
        score_noise = jax.random.randint(stage_key, (TOKENS, EXPERTS), 0, 1000)
        score_total = (score_noise + stage_bias) * EXPERTS + jnp.arange(EXPERTS)
        return lax.top_k(score_total, TOP)[1]

    expert_ids = lax.map(pick_stage, (stage_keys, hot_bias)).astype(jnp.int32)
    positions = jax.vmap(queue_pos)(expert_ids.reshape(STAGES * EP_DEVS, TOK_DEV * TOP))
    positions = positions.reshape(STAGES, NUM_SEQ, SEQ_LEN, TOP)
    owner_dev = (jnp.arange(NUM_SEQ) // SEQS_DEV)[None, :, None, None]
    slot_ids = jnp.where(positions < CAP_DEV, owner_dev * CAP_DEV + positions, -1).astype(jnp.int32)
    return expert_ids.reshape(STAGES, NUM_SEQ, SEQ_LEN, TOP), slot_ids


def setup_inputs(seed: int = 0, part: int = 0) -> dict:
    base_key = jax.random.key(seed)
    part_key = jax.random.fold_in(base_key, part)
    route_key, out_key, gain_key, mean_key, gate_key, resid_key = jax.random.split(part_key, 6)
    norm_key, q_key, k_key, v_key, o_key = jax.random.split(base_key, 5)
    expert_ids, slot_ids = draw_routing(route_key)
    expert_gain = jnp.exp(0.6 * jax.random.normal(gain_key, (STAGES, EXPERTS, 1, 1), jnp.float32))
    expert_mean = 0.7 * jax.random.normal(mean_key, (STAGES, EXPERTS, 1, D), jnp.float32)
    expert_out = (expert_mean + expert_gain * jax.random.normal(out_key, (STAGES, EXPERTS, CAPACITY, D), jnp.float32)).astype(jnp.bfloat16)
    gate_vals = jax.nn.softmax(2.0 * jax.random.normal(gate_key, (STAGES, NUM_SEQ, SEQ_LEN, TOP), jnp.float32), axis=-1).astype(jnp.float32)
    residual = jax.random.normal(resid_key, (STAGES, NUM_SEQ, SEQ_LEN, D), jnp.float32).astype(jnp.bfloat16)
    norm_scale = jnp.exp(0.5 * jax.random.normal(norm_key, (STAGES, D), jnp.float32)).astype(jnp.float32)
    w_query = (1.3 * D ** -0.5 * jax.random.normal(q_key, (STAGES, D, HEADS, HEAD), jnp.float32)).astype(jnp.bfloat16)
    w_key = (1.3 * D ** -0.5 * jax.random.normal(k_key, (STAGES, D, HEADS, HEAD), jnp.float32)).astype(jnp.bfloat16)
    w_value = (D ** -0.5 * jax.random.normal(v_key, (STAGES, D, HEADS, HEAD), jnp.float32)).astype(jnp.bfloat16)
    w_out = (3.0 * HIDDEN ** -0.5 * jax.random.normal(o_key, (STAGES, HEADS, HEAD, D), jnp.float32)).astype(jnp.bfloat16)
    return {'expert_out': expert_out, 'expert_ids': expert_ids, 'slot_ids': slot_ids, 'gate_vals': gate_vals, 'residual': residual, 'norm_scale': norm_scale, 'w_query': w_query, 'w_key': w_key, 'w_value': w_value, 'w_out': w_out}


def combine_rows(expert_table, ids_seq, slots_seq, gates_seq, resid_seq):
    kept_mask = slots_seq >= 0
    picked_rows = expert_table[ids_seq, jnp.where(kept_mask, slots_seq, 0)].astype(jnp.float32)
    gate_used = jnp.where(kept_mask, gates_seq, 0.0)
    merged = resid_seq.astype(jnp.float32) + jnp.sum(gate_used[..., None] * picked_rows, axis=1)
    return merged.astype(jnp.bfloat16)


def attn_block(merged, scale_vec, q_mat, k_mat, v_mat, o_mat):
    resid_f32 = merged.astype(jnp.float32)
    inv_rms = lax.rsqrt(jnp.mean(resid_f32 * resid_f32, axis=-1, keepdims=True) + NORM_EPS)
    normed_in = (resid_f32 * inv_rms * scale_vec).astype(jnp.bfloat16)

    def project(w_mat):
        product = jnp.dot(normed_in, w_mat, preferred_element_type=jnp.float32).astype(jnp.bfloat16)
        return product.reshape(SEQ_LEN, HEADS, HEAD).astype(jnp.float32)

    q_heads = project(q_mat)
    k_heads = project(k_mat)
    v_heads = project(v_mat)
    scores = jnp.einsum('qhe,khe->hqk', q_heads, k_heads) * HEAD ** -0.5
    causal = jnp.arange(SEQ_LEN)[:, None] >= jnp.arange(SEQ_LEN)[None, :]
    scores = jnp.where(causal, scores, -1e30)
    exp_scores = jnp.exp(scores - jnp.max(scores, axis=-1, keepdims=True))
    row_sums = jnp.sum(exp_scores, axis=-1)
    mixed_vals = jnp.einsum('hqk,khe->qhe', exp_scores.astype(jnp.bfloat16).astype(jnp.float32), v_heads)
    attn_out = (mixed_vals / row_sums.T[:, :, None]).astype(jnp.bfloat16).reshape(SEQ_LEN, HIDDEN)
    proj_out = jnp.dot(attn_out, o_mat, preferred_element_type=jnp.float32).astype(jnp.bfloat16)
    return (resid_f32 + proj_out.astype(jnp.float32)).astype(jnp.bfloat16)


def reference(expert_out, expert_ids, slot_ids, gate_vals, residual, norm_scale, w_query, w_key, w_value, w_out):
    def one_stage(stage_idx):
        prev_stage = (stage_idx + STAGES - 1) % STAGES
        expert_table = expert_out[prev_stage]
        scale_vec = norm_scale[stage_idx]
        q_mat = w_query[stage_idx].reshape(D, HIDDEN)
        k_mat = w_key[stage_idx].reshape(D, HIDDEN)
        v_mat = w_value[stage_idx].reshape(D, HIDDEN)
        o_mat = w_out[stage_idx].reshape(HIDDEN, D)

        def one_seq(seq_idx):
            merged = combine_rows(expert_table, expert_ids[prev_stage, seq_idx], slot_ids[prev_stage, seq_idx], gate_vals[prev_stage, seq_idx], residual[prev_stage, seq_idx])
            return attn_block(merged, scale_vec, q_mat, k_mat, v_mat, o_mat)

        return lax.map(one_seq, jnp.arange(NUM_SEQ))

    return lax.map(one_stage, jnp.arange(STAGES))
```

```python
import functools

import jax
import jax.numpy as jnp
from jax import lax
from jax.experimental import pallas as pl
from jax.experimental.pallas import tpu as pltpu
from jax.sharding import PartitionSpec as P

NORM_EPS = 1e-6
MESH = pl.DeviceIdType.MESH
TOK = 128
COL = 512


def combine_kernel(pp_size, o_hbm, tbl_in, h_hbm, out_hbm, o_buf, tbl, tblt, gmat, ysend, acc, yrecv, dsend, drecv, hz, zrecv,
                   o_sem, h_sem, t_ssem, t_rsem, d_ssem, d_rsem, credit, y_ssem, y_rsem, z_ssem, z_rsem, out_sem):
    experts, cap_all, width = o_hbm.shape
    cap = o_buf.shape[2]
    slots = experts * cap
    tokens = h_hbm.shape[0]
    n_tok, n_col = tokens // TOK, width // COL
    n_piece = n_tok * n_col
    me = lax.axis_index('ep')
    core = lax.rem(me, 2)
    row = me // 2
    partner = row * 2 + (1 - core)
    peer = (1 - row) * 2 + core
    diag = (1 - row) * 2 + (1 - core)
    owners = (diag, peer, partner, me)
    stage = lax.axis_index('pp')
    nxt = lax.rem(stage + 1, pp_size)
    prv = lax.rem(stage + pp_size - 1, pp_size)

    def o_copy(r, d):
        cols = pl.ds(d * COL, COL)
        return pltpu.make_async_copy(o_hbm.at[:, pl.ds(owners[r] * cap, cap), cols], o_buf.at[r, :, :, cols], o_sem.at[r, d])

    def h_copy(i):
        c, d = i // n_col, i % n_col
        return pltpu.make_async_copy(h_hbm.at[pl.ds(c * TOK, TOK), pl.ds(d * COL, COL)], hz.at[i], h_sem.at[i])

    def t_copy(r):
        return pltpu.make_async_remote_copy(src_ref=tbl_in, dst_ref=tbl.at[r], send_sem=t_ssem.at[r], recv_sem=t_rsem.at[r],
                                            device_id={'ep': owners[r]}, device_id_type=MESH)

    def d_copy(kind, d):
        return pltpu.make_async_remote_copy(src_ref=dsend.at[kind, d], dst_ref=drecv.at[kind, d], send_sem=d_ssem.at[kind, d],
                                            recv_sem=d_rsem.at[kind, d], device_id={'ep': partner}, device_id_type=MESH)

    def y_copy(i):
        return pltpu.make_async_remote_copy(src_ref=ysend.at[i], dst_ref=yrecv.at[i], send_sem=y_ssem.at[i], recv_sem=y_rsem.at[i],
                                            device_id={'ep': peer}, device_id_type=MESH)

    def z_copy(i):
        c, d = i // n_col, i % n_col
        return pltpu.make_async_remote_copy(src_ref=hz.at[i], dst_ref=zrecv.at[c, :, pl.ds(pl.multiple_of(d * COL, COL), COL)],
                                            send_sem=z_ssem.at[i], recv_sem=z_rsem.at[i], device_id={'pp': nxt}, device_id_type=MESH)

    for d in range(n_col):
        for r in range(4):
            o_copy(r, d).start()
    for i in range(n_piece):
        h_copy(i).start()

    barrier = pltpu.get_barrier_semaphore()
    for dev in (partner, peer, diag):
        pl.semaphore_signal(barrier, inc=1, device_id={'ep': dev}, device_id_type=MESH)
    for dev in (nxt, prv):
        pl.semaphore_signal(barrier, inc=1, device_id={'pp': dev}, device_id_type=MESH)
    pl.semaphore_wait(barrier, 5)

    for r in range(3):
        t_copy(r).start()
    tblt[3] = jnp.transpose(tbl_in[...])
    for r in range(3):
        t_copy(r).wait_recv()
        tblt[r] = jnp.transpose(tbl[r])

    base = (me * slots).astype(jnp.float32)

    def build(c):
        def rows(k, _):
            r, q = k // (TOK // 16), k % (TOK // 16)
            t = tblt[r, pl.ds(pl.multiple_of(c * TOK + q * 16, 16), 16), :]
            lane = lax.broadcasted_iota(jnp.int32, (16, slots), 1).astype(jnp.float32) + base
            g = jnp.zeros((16, slots), jnp.float32)
            for j in range(8):
                g = jnp.where(lane == t[:, j:j + 1], t[:, 8 + j:9 + j], g)
            g1 = g.astype(jnp.bfloat16)
            rest = g - g1.astype(jnp.float32)
            g2 = rest.astype(jnp.bfloat16)
            g3 = (rest - g2.astype(jnp.float32)).astype(jnp.bfloat16)
            at = pl.multiple_of(q * 16, 16)
            gmat[r, pl.ds(at, 16), :] = g1
            gmat[r, pl.ds(at + TOK, 16), :] = g2
            gmat[r, pl.ds(at + 2 * TOK, 16), :] = g3
            return 0
        lax.fori_loop(0, 4 * (TOK // 16), rows, 0)

    def partial(r, d):
        w = o_buf[r, :, :, pl.ds(pl.multiple_of(d * COL, COL), COL)].reshape(slots, COL)
        p = jnp.dot(gmat[r], w, preferred_element_type=jnp.float32)
        return p[:TOK] + p[TOK:2 * TOK] + p[2 * TOK:]

    def take_local(i):
        d = i % n_col
        d_copy(1, d).wait_recv()
        acc[i] += drecv[1, d]
        @pl.when(i // n_col < n_tok - 1)
        def _():
            pl.semaphore_signal(credit.at[1], inc=1, device_id={'ep': partner}, device_id_type=MESH)

    def finish(j):
        y_copy(j).wait_recv()
        hz[j] = (acc[j] + yrecv[j]).astype(jnp.bfloat16)
        z_copy(j).start()

    def step(i, _):
        c, d = i // n_col, i % n_col

        @pl.when(d == 0)
        def _():
            build(c)

        @pl.when(c == 0)
        def _():
            for r in range(4):
                o_copy(r, d).wait()

        @pl.when(c > 0)
        def _():
            for kind in range(2):
                d_copy(kind, d).wait_send()
                pl.semaphore_wait(credit.at[kind], 1)

        dsend[0, d] = partial(0, d)
        ysend[i] = partial(1, d)
        d_copy(0, d).start()
        dsend[1, d] = partial(2, d)
        h_copy(i).wait()
        acc[i] = partial(3, d) + hz[i].astype(jnp.float32)
        d_copy(1, d).start()
        d_copy(0, d).wait_recv()
        ysend[i] += drecv[0, d]

        @pl.when(c < n_tok - 1)
        def _():
            pl.semaphore_signal(credit.at[0], inc=1, device_id={'ep': partner}, device_id_type=MESH)

        @pl.when(i > 0)
        def _():
            take_local(i - 1)

        y_copy(i).start()

        @pl.when((i >= 3) & (i % 2 == 1))
        def _():
            finish((i - 3) // 2)
        return 0

    lax.fori_loop(0, n_piece, step, 0)
    take_local(n_piece - 1)

    def tail(j, _):
        finish(j)
        return 0
    lax.fori_loop((n_piece - 4) // 2 + 1, n_piece, tail, 0)

    def arrive(i, _):
        z_copy(i).wait_recv()
        y_copy(i).wait_send()
        z_copy(i).wait_send()
        return 0
    lax.fori_loop(0, n_piece, arrive, 0)
    out = pltpu.make_async_copy(zrecv, out_hbm, out_sem)
    out.start()
    for d in range(n_col):
        for kind in range(2):
            d_copy(kind, d).wait_send()
    for r in range(3):
        t_copy(r).wait_send()
    out.wait()


def exchange(pp_size, expert_out, table, resid, ep_size):
    experts, cap_all, width = expert_out.shape
    tokens = resid.shape[0]
    cap = cap_all // ep_size
    n_tok, n_col = tokens // TOK, width // COL
    n_piece = n_tok * n_col
    dma = pltpu.SemaphoreType.DMA
    return pl.pallas_call(
        functools.partial(combine_kernel, pp_size),
        out_shape=jax.ShapeDtypeStruct((n_tok, TOK, width), jnp.bfloat16),
        in_specs=[pl.BlockSpec(memory_space=pl.ANY), pl.BlockSpec(memory_space=pltpu.VMEM), pl.BlockSpec(memory_space=pl.ANY)],
        out_specs=pl.BlockSpec(memory_space=pl.ANY),
        scratch_shapes=[
            pltpu.VMEM((4, experts, cap, width), jnp.bfloat16),
            pltpu.VMEM((3, 16, tokens), jnp.float32),
            pltpu.VMEM((4, tokens, 16), jnp.float32),
            pltpu.VMEM((4, 3 * TOK, experts * cap), jnp.bfloat16),
            pltpu.VMEM((n_piece, TOK, COL), jnp.float32),
            pltpu.VMEM((n_piece, TOK, COL), jnp.float32),
            pltpu.VMEM((n_piece, TOK, COL), jnp.float32),
            pltpu.VMEM((2, n_col, TOK, COL), jnp.float32),
            pltpu.VMEM((2, n_col, TOK, COL), jnp.float32),
            pltpu.VMEM((n_piece, TOK, COL), jnp.bfloat16),
            pltpu.VMEM((n_tok, TOK, width), jnp.bfloat16),
            dma((4, n_col)), dma((n_piece,)), dma((3,)), dma((3,)), dma((2, n_col)), dma((2, n_col)),
            pltpu.SemaphoreType.REGULAR((2,)),
            dma((n_piece,)), dma((n_piece,)), dma((n_piece,)), dma((n_piece,)), dma,
        ],
        compiler_params=pltpu.CompilerParams(collective_id=0, has_side_effects=True, vmem_limit_bytes=64 * 1000 * 1024),
    )(expert_out, table, resid)


def attn_block(merged, scale_vec, w_query, w_key, w_value, w_out):
    head_dim = w_query.shape[-1]
    seq_len = merged.shape[1]
    resid_f32 = merged.astype(jnp.float32)
    inv_rms = lax.rsqrt(jnp.mean(resid_f32 * resid_f32, axis=-1, keepdims=True) + NORM_EPS)
    normed_in = (resid_f32 * inv_rms * scale_vec).astype(jnp.bfloat16)
    q_heads = jnp.einsum('bld,dhe->blhe', normed_in, w_query, preferred_element_type=jnp.float32).astype(jnp.bfloat16)
    k_heads = jnp.einsum('bld,dhe->blhe', normed_in, w_key, preferred_element_type=jnp.float32).astype(jnp.bfloat16)
    v_heads = jnp.einsum('bld,dhe->blhe', normed_in, w_value, preferred_element_type=jnp.float32).astype(jnp.bfloat16)
    scores = jnp.einsum('bqhe,bkhe->bhqk', q_heads, k_heads, preferred_element_type=jnp.float32) * (head_dim ** -0.5)
    causal = jnp.arange(seq_len)[:, None] >= jnp.arange(seq_len)[None, :]
    scores = jnp.where(causal, scores, -1e30)
    exp_scores = jnp.exp(scores - jnp.max(scores, axis=-1, keepdims=True))
    row_sums = jnp.sum(exp_scores, axis=-1)
    mixed_vals = jnp.einsum('bhqk,bkhe->bqhe', exp_scores.astype(jnp.bfloat16), v_heads, preferred_element_type=jnp.float32)
    attn_out = (mixed_vals / jnp.swapaxes(row_sums, -1, -2)[..., None]).astype(jnp.bfloat16)
    proj_out = jnp.einsum('crif,ife->cre', attn_out, w_out, preferred_element_type=jnp.float32).astype(jnp.bfloat16)
    return (resid_f32 + proj_out.astype(jnp.float32)).astype(jnp.bfloat16)


def solution(mesh):
    ep_size = mesh.shape['ep']
    pp_size = mesh.shape['pp']
    token_spec = P(('data', 'pp'), 'ep', None, None)
    weight_spec = P('pp', None, None, None)

    def body(expert_out, expert_ids, slot_ids, gate_vals, residual, norm_scale, w_query, w_key, w_value, w_out):
        local_experts, capacity, model_width = expert_out.shape[1:]
        cap_dev = capacity // ep_size
        ids, slots, gates = (jnp.swapaxes(a[0, 0], 0, 1) for a in (expert_ids, slot_ids, gate_vals))
        key = jnp.where(slots >= 0, ids * cap_dev + slots - lax.axis_index('ep') * cap_dev, -1)
        table = jnp.concatenate([key.astype(jnp.float32), gates], axis=0)
        arrived = exchange(pp_size, expert_out[0], table, residual[0, 0], ep_size).reshape(1, -1, model_width)
        result = attn_block(arrived, norm_scale[0], w_query[0], w_key[0], w_value[0], w_out[0])
        return result[None]

    return jax.shard_map(body, mesh=mesh, in_specs=(token_spec, token_spec, token_spec, token_spec, token_spec, P('pp', None), weight_spec, weight_spec, weight_spec, weight_spec), out_specs=token_spec, check_vma=False)
```

```python
import functools

import jax
import jax.numpy as jnp
from jax import lax
from jax.experimental import pallas as pl
from jax.experimental.pallas import tpu as pltpu
from jax.sharding import PartitionSpec as P

NORM_EPS = 1e-6
MESH = pl.DeviceIdType.MESH
TOK = 128
COL = 512
BLK = 128
NSLOT = 2


def stage_kernel(pp_size, heads, o_hbm, ids_in, slot_in, gate_in, h_hbm, scale_in, wq_hbm, wk_hbm, wv_hbm, wo_hbm, out_hbm,
                 arena, tids, tslot, tgate, tblt, gmat, ysend, acc, yrecv, dsend, drecv, hz, zrecv, stage_buf, wo_buf, qbuf, kbuf, vbuf, xbuf,
                 o_sem, h_sem, t_ssem, t_rsem, d_ssem, d_rsem, credit, y_ssem, y_rsem, z_ssem, z_rsem, s_sem, w_sem, out_sem):
    experts, cap_all, width = o_hbm.shape
    cap = cap_all // 4
    slots = experts * cap
    tokens = h_hbm.shape[0]
    head_dim = width // heads
    n_tok, n_col = tokens // TOK, width // COL
    n_piece = n_tok * n_col
    me = lax.axis_index('ep')
    core = lax.rem(me, 2)
    row = me // 2
    partner = row * 2 + (1 - core)
    peer = (1 - row) * 2 + core
    diag = (1 - row) * 2 + (1 - core)
    owners = (diag, peer, partner, me)
    stage = lax.axis_index('pp')
    nxt = lax.rem(stage + 1, pp_size)
    prv = lax.rem(stage + pp_size - 1, pp_size)

    def o_start(r, d):
        def one(e, _):
            pltpu.make_async_copy(o_hbm.at[e, pl.ds(owners[r] * cap, cap), pl.ds(d * COL, COL)],
                                  arena.at[pl.ds(pl.multiple_of(r * slots + e * cap, 16), cap), pl.ds(d * COL, COL)], o_sem.at[r, d]).start()
            return 0
        lax.fori_loop(0, experts, one, 0)

    def o_wait(r, d):
        view = arena.at[pl.ds(r * slots, slots), pl.ds(pl.multiple_of(d * COL, COL), COL)]
        pltpu.make_async_copy(view, view, o_sem.at[r, d]).wait()

    def h_copy(i):
        c, d = i // n_col, i % n_col
        return pltpu.make_async_copy(h_hbm.at[pl.ds(c * TOK, TOK), pl.ds(d * COL, COL)], hz.at[i], h_sem.at[i])

    tables = ((ids_in, tids), (slot_in, tslot), (gate_in, tgate))

    def t_copy(k, r):
        return pltpu.make_async_remote_copy(src_ref=tables[k][0], dst_ref=tables[k][1].at[r], send_sem=t_ssem.at[k, r],
                                            recv_sem=t_rsem.at[k, r], device_id={'ep': owners[r]}, device_id_type=MESH)

    def d_copy(kind, i):
        at = i % NSLOT
        return pltpu.make_async_remote_copy(src_ref=dsend.at[kind, at], dst_ref=drecv.at[kind, at], send_sem=d_ssem.at[kind, at],
                                            recv_sem=d_rsem.at[kind, at], device_id={'ep': partner}, device_id_type=MESH)

    def y_copy(i):
        return pltpu.make_async_remote_copy(src_ref=ysend.at[i], dst_ref=yrecv.at[i], send_sem=y_ssem.at[i], recv_sem=y_rsem.at[i],
                                            device_id={'ep': peer}, device_id_type=MESH)

    def z_copy(i):
        c, d = i // n_col, i % n_col
        return pltpu.make_async_remote_copy(src_ref=hz.at[i], dst_ref=zrecv.at[c, :, pl.ds(pl.multiple_of(d * COL, COL), COL)],
                                            send_sem=z_ssem.at[i], recv_sem=z_rsem.at[i], device_id={'pp': nxt}, device_id_type=MESH)

    raw = (wq_hbm, wk_hbm, wv_hbm)

    def s_copy(w, b):
        at = b % 2
        return pltpu.make_async_copy(raw[w].at[pl.ds(b * BLK, BLK)], stage_buf.at[at], s_sem.at[at])

    def w_copy(n):
        at = n % 2
        return pltpu.make_async_copy(wo_hbm.at[:, pl.ds(pl.multiple_of(n * COL, COL), COL)], wo_buf.at[at], w_sem.at[at])

    for r in range(4):
        o_start(r, 0)

    barrier = pltpu.get_barrier_semaphore()
    for dev in (partner, peer, diag):
        pl.semaphore_signal(barrier, inc=1, device_id={'ep': dev}, device_id_type=MESH)
    for dev in (nxt, prv):
        pl.semaphore_signal(barrier, inc=1, device_id={'pp': dev}, device_id_type=MESH)
    pl.semaphore_wait(barrier, 5)

    for r in range(3):
        for k in range(3):
            t_copy(k, r).start()

    def keyed(r, ids, slot, gate):
        key = jnp.where(slot >= 0, (ids - me * experts) * cap + (slot - owners[r] * cap), -1).astype(jnp.float32)
        tblt[r] = jnp.transpose(jnp.concatenate([key, gate], axis=0))

    keyed(3, ids_in[...], slot_in[...], gate_in[...])
    for r in range(3):
        for k in range(3):
            t_copy(k, r).wait_recv()
        keyed(r, tids[r], tslot[r], tgate[r])
    for d in range(1, n_col):
        for r in range(4):
            o_start(r, d)
    for i in range(n_piece):
        h_copy(i).start()
    s_copy(0, 0).start()
    w_copy(0).start()
    w_copy(1).start()

    groups = TOK // 16

    def build(c, first):
        def rows(k, _):
            r, q = first + k // groups, k % groups
            t = tblt[r, pl.ds(pl.multiple_of(c * TOK + q * 16, 16), 16), :]
            lane = lax.broadcasted_iota(jnp.int32, (16, slots), 1).astype(jnp.float32)
            g = jnp.zeros((16, slots), jnp.float32)
            for j in range(8):
                g = jnp.where(lane == t[:, j:j + 1], t[:, 8 + j:9 + j], g)
            g1 = g.astype(jnp.bfloat16)
            rest = g - g1.astype(jnp.float32)
            g2 = rest.astype(jnp.bfloat16)
            g3 = (rest - g2.astype(jnp.float32)).astype(jnp.bfloat16)
            at = pl.multiple_of(q * 16, 16)
            gmat[r, pl.ds(at, 16), :] = g1
            gmat[r, pl.ds(at + TOK, 16), :] = g2
            gmat[r, pl.ds(at + 2 * TOK, 16), :] = g3
            return 0
        lax.fori_loop(0, 2 * groups, rows, 0)

    def partial(r, d):
        w = arena[pl.ds(r * slots, slots), pl.ds(pl.multiple_of(d * COL, COL), COL)]
        p = jnp.dot(gmat[r], w, preferred_element_type=jnp.float32)
        return p[:TOK] + p[TOK:2 * TOK] + p[2 * TOK:]

    def give(kind, i):
        @pl.when(i < n_piece - NSLOT)
        def _():
            pl.semaphore_signal(credit.at[kind], inc=1, device_id={'ep': partner}, device_id_type=MESH)

    def take_local(i):
        d_copy(1, i).wait_recv()
        acc[i] += drecv[1, i % NSLOT]
        give(1, i)

    def finish(j):
        y_copy(j).wait_recv()
        hz[j] = (acc[j] + yrecv[j]).astype(jnp.bfloat16)
        z_copy(j).start()

    def step(i, _):
        c, d = i // n_col, i % n_col

        @pl.when(d == 0)
        def _():
            build(c, 0)

        @pl.when(c == 0)
        def _():
            for r in range(4):
                o_wait(r, d)

        @pl.when(i >= NSLOT)
        def _():
            for kind in range(2):
                d_copy(kind, i).wait_send()
                pl.semaphore_wait(credit.at[kind], 1)

        dsend[0, i % NSLOT] = partial(0, d)
        ysend[i] = partial(1, d)
        d_copy(0, i).start()

        @pl.when(d == 0)
        def _():
            build(c, 2)

        dsend[1, i % NSLOT] = partial(2, d)
        d_copy(0, i).wait_recv()
        ysend[i] += drecv[0, i % NSLOT]
        give(0, i)
        h_copy(i).wait()
        acc[i] = partial(3, d) + hz[i].astype(jnp.float32)
        y_copy(i).start()
        d_copy(1, i).start()

        @pl.when(i > 0)
        def _():
            take_local(i - 1)

        @pl.when((i >= 5) & (i % 2 == 1))
        def _():
            finish((i - 5) // 2)
        return 0

    lax.fori_loop(0, n_piece, step, 0)
    take_local(n_piece - 1)

    n_blk = width // BLK

    def relay(w):
        def block(b, _):
            at = b % 2
            s_copy(w, b).wait()

            @pl.when(b < n_blk - 1)
            def _():
                s_copy(w, b + 1).start()

            if w < 2:
                @pl.when(b == n_blk - 1)
                def _():
                    s_copy(w + 1, 0).start()

            def sub(k, _):
                rows = pl.multiple_of(k * 64, 64)
                arena[pl.ds(pl.multiple_of(w * width + b * BLK + rows, 64), 64), :] = stage_buf[at, pl.ds(rows, 64)].reshape(64, width)
                return 0
            lax.fori_loop(0, BLK // 64, sub, 0)
            return 0
        lax.fori_loop(0, n_blk, block, 0)

    def attend(c, hook):
        for d in range(n_col):
            z_copy(c * n_col + d).wait_recv()
        scale = scale_in[...]

        def norm(k, _):
            rows = pl.ds(pl.multiple_of(k * 16, 16), 16)
            x = zrecv[c, rows, :].astype(jnp.float32)
            inv = lax.rsqrt(jnp.mean(x * x, axis=-1, keepdims=True) + NORM_EPS)
            xbuf[rows, :] = (x * inv * scale).astype(jnp.bfloat16)
            return 0
        lax.fori_loop(0, TOK // 16, norm, 0)

        def project(n, _):
            cols = pl.ds(pl.multiple_of(n * COL, COL), COL)
            x = xbuf[...]
            qbuf[:, cols] = jnp.dot(x, arena[0:width, cols], preferred_element_type=jnp.float32).astype(jnp.bfloat16)
            kbuf[c * TOK:(c + 1) * TOK, cols] = jnp.dot(x, arena[width:2 * width, cols], preferred_element_type=jnp.float32).astype(jnp.bfloat16)
            vbuf[c * TOK:(c + 1) * TOK, cols] = jnp.dot(x, arena[2 * width:3 * width, cols], preferred_element_type=jnp.float32).astype(jnp.bfloat16)
            return 0
        lax.fori_loop(0, n_col, project, 0)
        hook(0)
        seen = (c + 1) * TOK
        q_at = lax.broadcasted_iota(jnp.int32, (TOK, seen), 0) + c * TOK
        k_at = lax.broadcasted_iota(jnp.int32, (TOK, seen), 1)
        causal = q_at >= k_at

        def head(h, _):
            for u in range(2):
                cols = pl.ds(pl.multiple_of((h * 2 + u) * head_dim, head_dim), head_dim)
                s = lax.dot_general(qbuf[:, cols], kbuf[0:seen, cols], (((1,), (1,)), ((), ())), preferred_element_type=jnp.float32)
                s = jnp.where(causal, s * (head_dim ** -0.5), -1e30)
                p = jnp.exp(s - jnp.max(s, axis=-1, keepdims=True))
                total = jnp.sum(p, axis=-1, keepdims=True)
                mixed = jnp.dot(p.astype(jnp.bfloat16), vbuf[0:seen, cols], preferred_element_type=jnp.float32)
                xbuf[:, cols] = (mixed / total).astype(jnp.bfloat16)
            return 0
        lax.fori_loop(0, heads // 2, head, 0)
        hook(1)

        def output(n, _):
            cols = pl.ds(pl.multiple_of(n * COL, COL), COL)
            w_copy(n).wait()
            proj = jnp.dot(xbuf[...], wo_buf[n % 2], preferred_element_type=jnp.float32).astype(jnp.bfloat16)
            zrecv[c, :, cols] = (zrecv[c, :, cols].astype(jnp.float32) + proj.astype(jnp.float32)).astype(jnp.bfloat16)
            if c < n_tok - 1:
                w_copy((n + 2) % n_col).start()
            else:
                @pl.when(n < n_col - 2)
                def _():
                    w_copy(n + 2).start()
            return 0
        lax.fori_loop(0, n_col, output, 0)
        pltpu.make_async_copy(zrecv.at[c], out_hbm.at[c], out_sem.at[c]).start()
        hook(2)

    relay(0)
    finish(6)
    relay(1)
    finish(7)
    relay(2)
    plan = {(0, 0): (8,), (0, 2): (9,), (1, 0): (10,), (1, 2): (11, 12), (2, 0): (13,), (2, 2): (14, 15)}
    for c in range(n_tok):
        def hook(at, c=c):
            for j in plan.get((c, at), ()):
                finish(j)
        attend(c, hook)

    def drain(i, _):
        y_copy(i).wait_send()
        z_copy(i).wait_send()
        return 0
    lax.fori_loop(0, n_piece, drain, 0)
    for i in range(NSLOT):
        for kind in range(2):
            d_copy(kind, i).wait_send()
    for r in range(3):
        for k in range(3):
            t_copy(k, r).wait_send()
    for c in range(n_tok):
        pltpu.make_async_copy(zrecv.at[c], out_hbm.at[c], out_sem.at[c]).wait()


def run_stage(pp_size, expert_out, ids, slot, gate, resid, scale, wq, wk, wv, wo):
    experts, cap_all, width = expert_out.shape
    tokens = resid.shape[0]
    heads = wq.shape[1]
    slots = experts * cap_all // 4
    n_tok, n_col = tokens // TOK, width // COL
    n_piece = n_tok * n_col
    dma = pltpu.SemaphoreType.DMA
    anyspace = pl.BlockSpec(memory_space=pl.ANY)
    vmem = pl.BlockSpec(memory_space=pltpu.VMEM)
    f32, bf16 = jnp.float32, jnp.bfloat16
    return pl.pallas_call(
        functools.partial(stage_kernel, pp_size, heads),
        out_shape=jax.ShapeDtypeStruct((n_tok, TOK, width), bf16),
        in_specs=[anyspace, vmem, vmem, vmem, anyspace, vmem, anyspace, anyspace, anyspace, anyspace],
        out_specs=anyspace,
        scratch_shapes=[
            pltpu.VMEM((max(4 * slots, 3 * width), width), bf16),
            pltpu.VMEM((3, 8, tokens), jnp.int32), pltpu.VMEM((3, 8, tokens), jnp.int32), pltpu.VMEM((3, 8, tokens), f32),
            pltpu.VMEM((4, tokens, 16), f32),
            pltpu.VMEM((4, 3 * TOK, slots), bf16),
            pltpu.VMEM((n_piece, TOK, COL), f32), pltpu.VMEM((n_piece, TOK, COL), f32), pltpu.VMEM((n_piece, TOK, COL), f32),
            pltpu.VMEM((2, NSLOT, TOK, COL), f32), pltpu.VMEM((2, NSLOT, TOK, COL), f32),
            pltpu.VMEM((n_piece, TOK, COL), bf16),
            pltpu.VMEM((n_tok, TOK, width), bf16),
            pltpu.VMEM((2, BLK, heads, width // heads), bf16),
            pltpu.VMEM((2, width, COL), bf16),
            pltpu.VMEM((TOK, width), bf16), pltpu.VMEM((tokens, width), bf16), pltpu.VMEM((tokens, width), bf16), pltpu.VMEM((TOK, width), bf16),
            dma((4, n_col)), dma((n_piece,)), dma((3, 3)), dma((3, 3)), dma((2, NSLOT)), dma((2, NSLOT)),
            pltpu.SemaphoreType.REGULAR((2,)),
            dma((n_piece,)), dma((n_piece,)), dma((n_piece,)), dma((n_piece,)), dma((2,)), dma((2,)), dma((n_tok,)),
        ],
        compiler_params=pltpu.CompilerParams(collective_id=0, has_side_effects=True, vmem_limit_bytes=67043328),
    )(expert_out, ids, slot, gate, resid, scale, wq, wk, wv, wo)


def solution(mesh):
    pp_size = mesh.shape['pp']
    token_spec = P(('data', 'pp'), 'ep', None, None)
    weight_spec = P('pp', None, None, None)

    def body(expert_out, expert_ids, slot_ids, gate_vals, residual, norm_scale, w_query, w_key, w_value, w_out):
        ids, slot, gate = (jnp.swapaxes(a[0, 0], 0, 1) for a in (expert_ids, slot_ids, gate_vals))
        width = expert_out.shape[-1]
        result = run_stage(pp_size, expert_out[0], ids, slot, gate, residual[0, 0], norm_scale, w_query[0], w_key[0], w_value[0], w_out[0].reshape(-1, width))
        return result.reshape(residual.shape)

    return jax.shard_map(body, mesh=mesh, in_specs=(token_spec, token_spec, token_spec, token_spec, token_spec, P('pp', None), weight_spec, weight_spec, weight_spec, weight_spec), out_specs=token_spec, check_vma=False)
```

```python
import functools

import jax
import jax.numpy as jnp
from jax import lax
from jax.experimental import pallas as pl
from jax.experimental.pallas import tpu as pltpu
from jax.sharding import PartitionSpec as P

NORM_EPS = 1e-6
MESH = pl.DeviceIdType.MESH
TOK = 128
COL = 512
WIDE = 1024
BLK = 128
STAGED = 6
OUT = 256
WSLOT = 6
GROUP = 8


def stage_kernel(pp_size, heads, o_hbm, ids_in, slot_in, gate_in, h_hbm, scale_in, wq_hbm, wk_hbm, wv_hbm, wo_hbm, out_hbm,
                 arena, tids, tslot, tgate, tblt, gate_a, gate_b, ysend, acc, yrecv, dsend, drecv, hz, zrecv, stage_buf, wo_buf, qbuf, kbuf, vbuf, xbuf,
                 o_sem, h_sem, t_ssem, t_rsem, d_ssem, d_rsem, credit, y_ssem, y_rsem, z_ssem, z_rsem, s_sem, w_sem, out_sem):
    experts, cap_all, width = o_hbm.shape
    cap = cap_all // 4
    slots = experts * cap
    tokens = h_hbm.shape[0]
    head_dim = width // heads
    n_tok, n_col = tokens // TOK, width // COL
    n_piece = n_tok * n_col
    n_out = width // OUT
    gates = (gate_b, gate_a)
    me = lax.axis_index('ep')
    core = lax.rem(me, 2)
    row = me // 2
    partner = row * 2 + (1 - core)
    peer = (1 - row) * 2 + core
    diag = (1 - row) * 2 + (1 - core)
    owners = (diag, peer, partner, me)
    stage = lax.axis_index('pp')
    nxt = lax.rem(stage + 1, pp_size)
    prv = lax.rem(stage + pp_size - 1, pp_size)

    def o_start(r):
        def one(e, _):
            pltpu.make_async_copy(o_hbm.at[e, pl.ds(owners[r] * cap, cap)],
                                  arena.at[pl.ds(pl.multiple_of(r * slots + e * cap, 16), cap)], o_sem.at[r]).start()
            return 0
        lax.fori_loop(0, experts, one, 0)

    def o_wait(r):
        view = arena.at[pl.ds(r * slots, slots)]
        pltpu.make_async_copy(view, view, o_sem.at[r]).wait()

    def h_copy(i):
        c, d = i // n_col, i % n_col
        return pltpu.make_async_copy(h_hbm.at[pl.ds(c * TOK, TOK), pl.ds(d * COL, COL)], hz.at[i], h_sem.at[i])

    tables = ((ids_in, tids), (slot_in, tslot), (gate_in, tgate))

    def t_copy(k, r):
        return pltpu.make_async_remote_copy(src_ref=tables[k][0], dst_ref=tables[k][1].at[r], send_sem=t_ssem.at[k, r],
                                            recv_sem=t_rsem.at[k, r], device_id={'ep': owners[r]}, device_id_type=MESH)

    def d_copy(d):
        return pltpu.make_async_remote_copy(src_ref=dsend.at[d], dst_ref=drecv.at[d], send_sem=d_ssem.at[d],
                                            recv_sem=d_rsem.at[d], device_id={'ep': partner}, device_id_type=MESH)

    def y_copy(i):
        return pltpu.make_async_remote_copy(src_ref=ysend.at[i], dst_ref=yrecv.at[i], send_sem=y_ssem.at[i], recv_sem=y_rsem.at[i],
                                            device_id={'ep': peer}, device_id_type=MESH)

    def z_copy(i):
        c, d = i // n_col, i % n_col
        return pltpu.make_async_remote_copy(src_ref=hz.at[i], dst_ref=zrecv.at[c, :, pl.ds(pl.multiple_of(d * COL, COL), COL)],
                                            send_sem=z_ssem.at[i], recv_sem=z_rsem.at[i], device_id={'pp': nxt}, device_id_type=MESH)

    raw = (wq_hbm, wk_hbm, wv_hbm)

    n_blk = width // BLK

    def s_copy(w, b, at):
        return pltpu.make_async_copy(raw[w].at[pl.ds(b * BLK, BLK)], stage_buf.at[at], s_sem.at[at])

    def s_start(m):
        for w in range(3):
            @pl.when(m // n_blk == w)
            def _():
                s_copy(w, m % n_blk, m % STAGED).start()

    def w_copy(n):
        at = n % WSLOT
        return pltpu.make_async_copy(wo_hbm.at[:, pl.ds(pl.multiple_of(n % n_out * OUT, OUT), OUT)], wo_buf.at[at], w_sem.at[at])

    def keyed(r, ids, slot, gate):
        key = jnp.where(slot >= 0, (ids - me * experts) * cap + (slot - owners[r] * cap), -1).astype(jnp.float32)
        tblt[:, r * 16:(r + 1) * 16] = jnp.transpose(jnp.concatenate([key, gate], axis=0))

    groups = TOK // 16

    def build(c, r, q):
        t = tblt[pl.ds(pl.multiple_of(c * TOK + q * 16, 16), 16), r * 16:(r + 1) * 16]
        lane = lax.broadcasted_iota(jnp.int32, (16, slots), 1).astype(jnp.float32)
        g = jnp.zeros((16, slots), jnp.float32)
        for j in range(8):
            g = jnp.where(lane == t[:, j:j + 1], t[:, 8 + j:9 + j], g)
        g1 = g.astype(jnp.bfloat16)
        rest = g - g1.astype(jnp.float32)
        g2 = rest.astype(jnp.bfloat16)
        g3 = (rest - g2.astype(jnp.float32)).astype(jnp.bfloat16)
        at = pl.multiple_of(q * 16, 16)
        dst = gates[r % 2]
        dst[pl.ds(at, 16), :] = g1
        dst[pl.ds(at + TOK, 16), :] = g2
        dst[pl.ds(at + 2 * TOK, 16), :] = g3

    def build_all(c, r):
        def one(q, _):
            build(c, r, q)
            return 0
        lax.fori_loop(0, groups, one, 0)

    halves = width // WIDE
    per = WIDE // COL

    def phase(c, r, ahead, before, use):
        def half(h, _):
            before(h)
            w = arena[r * slots:(r + 1) * slots, pl.ds(pl.multiple_of(h * WIDE, WIDE), WIDE)]
            p = jnp.dot(gates[r % 2][...], w, preferred_element_type=jnp.float32)
            total = p[:TOK] + p[TOK:2 * TOK] + p[2 * TOK:]
            if ahead is not None:
                for q in range(groups // halves):
                    build(*ahead, h * (groups // halves) + q)
            for u in range(per):
                use(h * per + u, total[:, u * COL:(u + 1) * COL])
            return 0
        lax.fori_loop(0, halves, half, 0)

    def give():
        pl.semaphore_signal(credit, inc=1, device_id={'ep': partner}, device_id_type=MESH)

    def hold(d):
        d_copy(d).wait_send()
        pl.semaphore_wait(credit, 1)

    def send_core(d, value):
        dsend[d] = value
        d_copy(d).start()

    def self_role(c, ahead):
        def before(h):
            for u in range(per):
                h_copy(c * n_col + h * per + u).wait()

        def use(d, value):
            i = c * n_col + d
            acc[i] = value + hz[i].astype(jnp.float32)
        phase(c, 3, ahead, before, use)

    def take_local(c):
        def one(d, _):
            d_copy(d).wait_recv()
            acc[c * n_col + d] += drecv[d]

            @pl.when(c < n_tok - 1)
            def _():
                give()
            return 0
        lax.fori_loop(0, n_col, one, 0)

    def finish(j):
        y_copy(j).wait_recv()
        hz[j] = (acc[j] + yrecv[j]).astype(jnp.bfloat16)
        z_copy(j).start()

    o_start(3)
    o_start(0)
    barrier = pltpu.get_barrier_semaphore()
    for dev in (partner, peer, diag):
        pl.semaphore_signal(barrier, inc=1, device_id={'ep': dev}, device_id_type=MESH)
    for dev in (nxt, prv):
        pl.semaphore_signal(barrier, inc=1, device_id={'pp': dev}, device_id_type=MESH)
    for i in range(n_col):
        h_copy(i).start()
    keyed(3, ids_in[...], slot_in[...], gate_in[...])
    pl.semaphore_wait(barrier, 5)
    for r in range(3):
        for k in range(3):
            t_copy(k, r).start()
    build_all(0, 3)
    o_start(1)
    o_start(2)
    o_wait(3)
    self_role(0, None)
    for r in range(3):
        for k in range(3):
            t_copy(k, r).wait_recv()
        keyed(r, tids[r], tslot[r], tgate[r])
    build_all(0, 0)
    for r in range(3):
        o_wait(r)

    def rest_h(i, _):
        h_copy(i).start()
        return 0
    lax.fori_loop(n_col, n_piece, rest_h, 0)
    for m in range(STAGED - 1):
        s_copy(0, m, m).start()
    for n in range(WSLOT):
        w_copy(n).start()

    def chunk(c, _):
        def hold0(h):
            @pl.when(c > 0)
            def _():
                for u in range(per):
                    hold(h * per + u)
        phase(c, 0, (c, 1), hold0, send_core)

        def got(h):
            for u in range(per):
                d_copy(h * per + u).wait_recv()

        def merge(d, value):
            i = c * n_col + d
            ysend[i] = value + drecv[d]
            give()
            y_copy(i).start()
        phase(c, 1, (c, 2), got, merge)

        def hold2(h):
            for u in range(per):
                hold(h * per + u)
        phase(c, 2, (lax.rem(c + 1, n_tok), 3), hold2, send_core)

        @pl.when(c < n_tok - 1)
        def _():
            self_role(c + 1, (c + 1, 0))
        take_local(c)

        @pl.when(c > 0)
        def _():
            finish(2 * c - 2)
            finish(2 * c - 1)
        return 0

    with jax.named_scope('combine'):
        lax.fori_loop(0, n_tok, chunk, 0)

    def relay(w):
        def block(b, _):
            m = w * n_blk + b
            at = m % STAGED
            s_copy(w, b, at).wait()

            @pl.when(m + STAGED - 1 < 3 * n_blk)
            def _():
                s_start(m + STAGED - 1)

            def sub(k, _):
                rows = pl.multiple_of(k * 64, 64)
                arena[pl.ds(pl.multiple_of(w * width + b * BLK + rows, 64), 64), :] = stage_buf[at, pl.ds(rows, 64)].reshape(64, width)
                return 0
            lax.fori_loop(0, BLK // 64, sub, 0)
            return 0
        lax.fori_loop(0, n_blk, block, 0)

    def attend(c, hook):
        with jax.named_scope('zwait'):
            for d in range(n_col):
                z_copy(c * n_col + d).wait_recv()
        scale = scale_in[...]

        def norm(k, _):
            rows = pl.ds(pl.multiple_of(k * 16, 16), 16)
            x = zrecv[c, rows, :].astype(jnp.float32)
            inv = lax.rsqrt(jnp.mean(x * x, axis=-1, keepdims=True) + NORM_EPS)
            xbuf[rows, :] = (x * inv * scale).astype(jnp.bfloat16)
            return 0
        lax.fori_loop(0, TOK // 16, norm, 0)

        def project(n, _):
            cols = pl.ds(pl.multiple_of(n * COL, COL), COL)
            x = xbuf[...]
            qbuf[:, cols] = jnp.dot(x, arena[0:width, cols], preferred_element_type=jnp.float32).astype(jnp.bfloat16)
            kbuf[c * TOK:(c + 1) * TOK, cols] = jnp.dot(x, arena[width:2 * width, cols], preferred_element_type=jnp.float32).astype(jnp.bfloat16)
            vbuf[c * TOK:(c + 1) * TOK, cols] = jnp.dot(x, arena[2 * width:3 * width, cols], preferred_element_type=jnp.float32).astype(jnp.bfloat16)
            return 0
        with jax.named_scope('project'):
            lax.fori_loop(0, n_col, project, 0)
        hook(0)
        seen = (c + 1) * TOK
        q_at = lax.broadcasted_iota(jnp.int32, (TOK, seen), 0) + c * TOK
        k_at = lax.broadcasted_iota(jnp.int32, (TOK, seen), 1)
        causal = q_at >= k_at

        def head(h, _):
            cols = [pl.ds(pl.multiple_of((h * GROUP + u) * head_dim, head_dim), head_dim) for u in range(GROUP)]
            logits = [lax.dot_general(qbuf[:, at], kbuf[0:seen, at], (((1,), (1,)), ((), ())), preferred_element_type=jnp.float32) for at in cols]
            logits = [jnp.where(causal, s * (head_dim ** -0.5), -1e30) for s in logits]
            probs = [jnp.exp(s - jnp.max(s, axis=-1, keepdims=True)) for s in logits]
            sums = [jnp.sum(p, axis=-1, keepdims=True) for p in probs]
            mixed = [jnp.dot(p.astype(jnp.bfloat16), vbuf[0:seen, at], preferred_element_type=jnp.float32) for p, at in zip(probs, cols)]
            for at, m, t in zip(cols, mixed, sums):
                xbuf[:, at] = (m / t).astype(jnp.bfloat16)
            return 0
        with jax.named_scope('heads'):
            lax.fori_loop(0, heads // GROUP, head, 0)
        hook(1)

        def output(k, _):
            for u in range(2):
                n = c * n_out + 2 * k + u
                cols = pl.ds(pl.multiple_of((2 * k + u) * OUT, OUT), OUT)
                w_copy(n).wait()
                proj = jnp.dot(xbuf[...], wo_buf[n % WSLOT], preferred_element_type=jnp.float32).astype(jnp.bfloat16)
                zrecv[c, :, cols] = (zrecv[c, :, cols].astype(jnp.float32) + proj.astype(jnp.float32)).astype(jnp.bfloat16)

                @pl.when(n + WSLOT < n_tok * n_out)
                def _():
                    w_copy(n + WSLOT).start()
            return 0
        with jax.named_scope('output'):
            lax.fori_loop(0, n_out // 2, output, 0)
        pltpu.make_async_copy(zrecv.at[c], out_hbm.at[c], out_sem.at[c]).start()
        hook(2)

    with jax.named_scope('relay'):
        relay(0)
        finish(6)
        relay(1)
        relay(2)
    finish(7)
    plan = {(0, 0): (8,), (0, 2): (9,), (1, 0): (10,), (1, 2): (11, 12), (2, 0): (13,), (2, 2): (14, 15)}
    for c in range(n_tok):
        def hook(at, c=c):
            for j in plan.get((c, at), ()):
                with jax.named_scope('fin'):
                    finish(j)
        with jax.named_scope('attend'):
            attend(c, hook)

    def drain(i, _):
        y_copy(i).wait_send()
        z_copy(i).wait_send()
        return 0
    lax.fori_loop(0, n_piece, drain, 0)
    for d in range(n_col):
        d_copy(d).wait_send()
    for r in range(3):
        for k in range(3):
            t_copy(k, r).wait_send()
    for c in range(n_tok):
        pltpu.make_async_copy(zrecv.at[c], out_hbm.at[c], out_sem.at[c]).wait()


def run_stage(pp_size, expert_out, ids, slot, gate, resid, scale, wq, wk, wv, wo):
    experts, cap_all, width = expert_out.shape
    tokens = resid.shape[0]
    heads = wq.shape[1]
    slots = experts * cap_all // 4
    n_tok, n_col = tokens // TOK, width // COL
    n_piece = n_tok * n_col
    dma = pltpu.SemaphoreType.DMA
    anyspace = pl.BlockSpec(memory_space=pl.ANY)
    vmem = pl.BlockSpec(memory_space=pltpu.VMEM)
    f32, bf16 = jnp.float32, jnp.bfloat16
    return pl.pallas_call(
        functools.partial(stage_kernel, pp_size, heads),
        out_shape=jax.ShapeDtypeStruct((n_tok, TOK, width), bf16),
        in_specs=[anyspace, vmem, vmem, vmem, anyspace, vmem, anyspace, anyspace, anyspace, anyspace],
        out_specs=anyspace,
        scratch_shapes=[
            pltpu.VMEM((max(4 * slots, 3 * width), width), bf16),
            pltpu.VMEM((3, 8, tokens), jnp.int32), pltpu.VMEM((3, 8, tokens), jnp.int32), pltpu.VMEM((3, 8, tokens), f32),
            pltpu.VMEM((tokens, 64), f32),
            pltpu.VMEM((3 * TOK, slots), bf16), pltpu.VMEM((3 * TOK, slots), bf16),
            pltpu.VMEM((n_piece, TOK, COL), f32), pltpu.VMEM((n_piece, TOK, COL), f32), pltpu.VMEM((n_piece, TOK, COL), f32),
            pltpu.VMEM((n_col, TOK, COL), f32), pltpu.VMEM((n_col, TOK, COL), f32),
            pltpu.VMEM((n_piece, TOK, COL), bf16),
            pltpu.VMEM((n_tok, TOK, width), bf16),
            pltpu.VMEM((STAGED, BLK, heads, width // heads), bf16),
            pltpu.VMEM((WSLOT, width, OUT), bf16),
            pltpu.VMEM((TOK, width), bf16), pltpu.VMEM((tokens, width), bf16), pltpu.VMEM((tokens, width), bf16), pltpu.VMEM((TOK, width), bf16),
            dma((4,)), dma((n_piece,)), dma((3, 3)), dma((3, 3)), dma((n_col,)), dma((n_col,)),
            pltpu.SemaphoreType.REGULAR,
            dma((n_piece,)), dma((n_piece,)), dma((n_piece,)), dma((n_piece,)), dma((STAGED,)), dma((WSLOT,)), dma((n_tok,)),
        ],
        compiler_params=pltpu.CompilerParams(collective_id=0, has_side_effects=True, vmem_limit_bytes=67043328),
    )(expert_out, ids, slot, gate, resid, scale, wq, wk, wv, wo)


def solution(mesh):
    pp_size = mesh.shape['pp']
    token_spec = P(('data', 'pp'), 'ep', None, None)
    weight_spec = P('pp', None, None, None)

    def body(expert_out, expert_ids, slot_ids, gate_vals, residual, norm_scale, w_query, w_key, w_value, w_out):
        ids, slot, gate = (jnp.swapaxes(a[0, 0], 0, 1) for a in (expert_ids, slot_ids, gate_vals))
        width = expert_out.shape[-1]
        result = run_stage(pp_size, expert_out[0], ids, slot, gate, residual[0, 0], norm_scale, w_query[0], w_key[0], w_value[0], w_out[0].reshape(-1, width))
        return result.reshape(residual.shape)

    return jax.shard_map(body, mesh=mesh, in_specs=(token_spec, token_spec, token_spec, token_spec, token_spec, P('pp', None), weight_spec, weight_spec, weight_spec, weight_spec), out_specs=token_spec, check_vma=False)
```

```python
import functools

import jax
import jax.numpy as jnp
from jax import lax
from jax.experimental import pallas as pl
from jax.experimental.pallas import tpu as pltpu
from jax.sharding import PartitionSpec as P

NORM_EPS = 1e-6
MESH = pl.DeviceIdType.MESH
TOK = 128
COL = 512
WIDE = 1024
BLK = 128
STAGED = 6
OUT = 256
WSLOT = 6
GROUP = 8
PARTS = 4


def stage_kernel(pp_size, heads, o_hbm, ids_in, slot_in, gate_in, h_hbm, scale_in, wq_hbm, wk_hbm, wv_hbm, wo_hbm, out_hbm,
                 arena, tids, tslot, tgate, tblt, gate_a, gate_b, ysend, acc, yrecv, dsend, drecv, hz, zrecv, stage_buf, wo_buf, qbuf, kbuf, vbuf, xbuf,
                 o_sem, h_sem, t_ssem, t_rsem, d_ssem, d_rsem, credit, y_ssem, y_rsem, z_ssem, z_rsem, yp_ssem, yp_rsem, zp_ssem, zp_rsem, s_sem, w_sem, out_sem):
    experts, cap_all, width = o_hbm.shape
    cap = cap_all // 4
    slots = experts * cap
    tokens = h_hbm.shape[0]
    head_dim = width // heads
    n_tok, n_col = tokens // TOK, width // COL
    n_piece = n_tok * n_col
    n_out = width // OUT
    gates = (gate_b, gate_a)
    me = lax.axis_index('ep')
    core = lax.rem(me, 2)
    row = me // 2
    partner = row * 2 + (1 - core)
    peer = (1 - row) * 2 + core
    diag = (1 - row) * 2 + (1 - core)
    owners = (diag, peer, partner, me)
    stage = lax.axis_index('pp')
    nxt = lax.rem(stage + 1, pp_size)
    prv = lax.rem(stage + pp_size - 1, pp_size)

    def o_start(r):
        def one(e, _):
            pltpu.make_async_copy(o_hbm.at[e, pl.ds(owners[r] * cap, cap)],
                                  arena.at[pl.ds(pl.multiple_of(r * slots + e * cap, 16), cap)], o_sem.at[r]).start()
            return 0
        lax.fori_loop(0, experts, one, 0)

    def o_wait(r):
        view = arena.at[pl.ds(r * slots, slots)]
        pltpu.make_async_copy(view, view, o_sem.at[r]).wait()

    def h_copy(i):
        c, d = i // n_col, i % n_col
        return pltpu.make_async_copy(h_hbm.at[pl.ds(c * TOK, TOK), pl.ds(d * COL, COL)], hz.at[i], h_sem.at[i])

    tables = ((ids_in, tids), (slot_in, tslot), (gate_in, tgate))

    def t_copy(k, r):
        return pltpu.make_async_remote_copy(src_ref=tables[k][0], dst_ref=tables[k][1].at[r], send_sem=t_ssem.at[k, r],
                                            recv_sem=t_rsem.at[k, r], device_id={'ep': owners[r]}, device_id_type=MESH)

    def d_copy(d):
        return pltpu.make_async_remote_copy(src_ref=dsend.at[d], dst_ref=drecv.at[d], send_sem=d_ssem.at[d],
                                            recv_sem=d_rsem.at[d], device_id={'ep': partner}, device_id_type=MESH)

    def y_copy(i):
        return pltpu.make_async_remote_copy(src_ref=ysend.at[i], dst_ref=yrecv.at[i], send_sem=y_ssem.at[i], recv_sem=y_rsem.at[i],
                                            device_id={'ep': peer}, device_id_type=MESH)

    def z_copy(i):
        c, d = i // n_col, i % n_col
        return pltpu.make_async_remote_copy(src_ref=hz.at[i], dst_ref=zrecv.at[c, :, pl.ds(pl.multiple_of(d * COL, COL), COL)],
                                            send_sem=z_ssem.at[i], recv_sem=z_rsem.at[i], device_id={'pp': nxt}, device_id_type=MESH)

    last = n_piece - 1
    thin = TOK // PARTS

    def y_part(k):
        rows = pl.ds(k * thin, thin)
        return pltpu.make_async_remote_copy(src_ref=ysend.at[last, rows], dst_ref=yrecv.at[last, rows], send_sem=yp_ssem.at[k],
                                            recv_sem=yp_rsem.at[k], device_id={'ep': peer}, device_id_type=MESH)

    def z_part(k):
        rows = pl.ds(k * thin, thin)
        return pltpu.make_async_remote_copy(src_ref=hz.at[last, rows], dst_ref=zrecv.at[n_tok - 1, rows, pl.ds(width - COL, COL)],
                                            send_sem=zp_ssem.at[k], recv_sem=zp_rsem.at[k], device_id={'pp': nxt}, device_id_type=MESH)

    raw = (wq_hbm, wk_hbm, wv_hbm)

    n_blk = width // BLK

    def s_copy(w, b, at):
        return pltpu.make_async_copy(raw[w].at[pl.ds(b * BLK, BLK)], stage_buf.at[at], s_sem.at[at])

    def s_start(m):
        for w in range(3):
            @pl.when(m // n_blk == w)
            def _():
                s_copy(w, m % n_blk, m % STAGED).start()

    def w_copy(n):
        at = n % WSLOT
        return pltpu.make_async_copy(wo_hbm.at[:, pl.ds(pl.multiple_of(n % n_out * OUT, OUT), OUT)], wo_buf.at[at], w_sem.at[at])

    def keyed(r, ids, slot, gate):
        key = jnp.where(slot >= 0, (ids - me * experts) * cap + (slot - owners[r] * cap), -1).astype(jnp.float32)
        tblt[:, r * 16:(r + 1) * 16] = jnp.transpose(jnp.concatenate([key, gate], axis=0))

    groups = TOK // 16

    def build(c, r, q):
        t = tblt[pl.ds(pl.multiple_of(c * TOK + q * 16, 16), 16), r * 16:(r + 1) * 16]
        lane = lax.broadcasted_iota(jnp.int32, (16, slots), 1).astype(jnp.float32)
        g = jnp.zeros((16, slots), jnp.float32)
        for j in range(8):
            g = jnp.where(lane == t[:, j:j + 1], t[:, 8 + j:9 + j], g)
        g1 = g.astype(jnp.bfloat16)
        rest = g - g1.astype(jnp.float32)
        g2 = rest.astype(jnp.bfloat16)
        g3 = (rest - g2.astype(jnp.float32)).astype(jnp.bfloat16)
        at = pl.multiple_of(q * 16, 16)
        dst = gates[r % 2]
        dst[pl.ds(at, 16), :] = g1
        dst[pl.ds(at + TOK, 16), :] = g2
        dst[pl.ds(at + 2 * TOK, 16), :] = g3

    def build_all(c, r):
        def one(q, _):
            build(c, r, q)
            return 0
        lax.fori_loop(0, groups, one, 0)

    halves = width // WIDE
    per = WIDE // COL

    def dot_role(r, h):
        w = arena[r * slots:(r + 1) * slots, h * WIDE:(h + 1) * WIDE]
        p = jnp.dot(gates[r % 2][...], w, preferred_element_type=jnp.float32)
        total = p[:TOK] + p[TOK:2 * TOK] + p[2 * TOK:]
        return [(h * per + u, total[:, u * COL:(u + 1) * COL]) for u in range(per)]

    def build_now(c, r):
        for q in range(groups):
            build(c, r, q)

    def give():
        pl.semaphore_signal(credit, inc=1, device_id={'ep': partner}, device_id_type=MESH)

    def hold(d):
        d_copy(d).wait_send()
        pl.semaphore_wait(credit, 1)

    def finish(j):
        y_copy(j).wait_recv()
        hz[j] = (acc[j] + yrecv[j]).astype(jnp.bfloat16)
        z_copy(j).start()

    def finish_last():
        for k in range(PARTS):
            rows = pl.ds(k * thin, thin)
            y_part(k).wait_recv()
            hz[last, rows] = (acc[last, rows] + yrecv[last, rows]).astype(jnp.bfloat16)
            z_part(k).start()

    o_start(0)
    barrier = pltpu.get_barrier_semaphore()
    for dev in (partner, peer, diag):
        pl.semaphore_signal(barrier, inc=1, device_id={'ep': dev}, device_id_type=MESH)
    for dev in (nxt, prv):
        pl.semaphore_signal(barrier, inc=1, device_id={'pp': dev}, device_id_type=MESH)
    for i in range(n_col):
        h_copy(i).start()
    o_start(1)
    pl.semaphore_wait(barrier, 5)
    for r in range(3):
        for k in range(3):
            t_copy(k, r).start()
    keyed(3, ids_in[...], slot_in[...], gate_in[...])
    o_start(2)
    o_start(3)
    for r in range(3):
        for k in range(3):
            t_copy(k, r).wait_recv()
        keyed(r, tids[r], tslot[r], tgate[r])
    build_all(0, 0)
    for r in range(4):
        o_wait(r)

    def rest_h(i, _):
        h_copy(i).start()
        return 0
    lax.fori_loop(n_col, n_piece, rest_h, 0)
    for m in range(STAGED - 1):
        s_copy(0, m, m).start()
    for n in range(WSLOT):
        w_copy(n).start()

    def chunk(c, _):
        for h in range(halves):
            @pl.when(c > 0)
            def _():
                for u in range(per):
                    hold(h * per + u)
            for d, value in dot_role(0, h):
                dsend[d] = value
            if h == 0:
                build_now(c, 1)
            for u in range(per):
                d_copy(h * per + u).start()
            for d, value in dot_role(1, h):
                ysend[c * n_col + d] = value
            if h == halves - 1:
                build_now(c, 2)
            for u in range(per):
                d = h * per + u
                i = c * n_col + d
                d_copy(d).wait_recv()
                ysend[i] += drecv[d]
                give()
                if d < n_col - 1:
                    y_copy(i).start()
                else:
                    @pl.when(c < n_tok - 1)
                    def _():
                        y_copy(i).start()

                    @pl.when(c == n_tok - 1)
                    def _():
                        for k in range(PARTS):
                            y_part(k).start()
        for h in range(halves):
            for u in range(per):
                hold(h * per + u)
            for d, value in dot_role(2, h):
                dsend[d] = value
            if h == 0:
                build_now(c, 3)
            for u in range(per):
                d_copy(h * per + u).start()
                h_copy(c * n_col + h * per + u).wait()
            for d, value in dot_role(3, h):
                i = c * n_col + d
                acc[i] = value + hz[i].astype(jnp.float32)
            if h == halves - 1:
                build_now(lax.rem(c + 1, n_tok), 0)
            for u in range(per):
                d = h * per + u
                d_copy(d).wait_recv()
                acc[c * n_col + d] += drecv[d]

                @pl.when(c < n_tok - 1)
                def _():
                    give()

        @pl.when(c > 0)
        def _():
            finish(2 * c - 2)
            finish(2 * c - 1)
        return 0

    with jax.named_scope('combine'):
        lax.fori_loop(0, n_tok, chunk, 0)

    def relay(w):
        def block(b, _):
            m = w * n_blk + b
            at = m % STAGED
            s_copy(w, b, at).wait()

            @pl.when(m + STAGED - 1 < 3 * n_blk)
            def _():
                s_start(m + STAGED - 1)

            def sub(k, _):
                rows = pl.multiple_of(k * 64, 64)
                arena[pl.ds(pl.multiple_of(w * width + b * BLK + rows, 64), 64), :] = stage_buf[at, pl.ds(rows, 64)].reshape(64, width)
                return 0
            lax.fori_loop(0, BLK // 64, sub, 0)
            return 0
        lax.fori_loop(0, n_blk, block, 0)

    def attend(c, hook):
        with jax.named_scope('zwait'):
            for d in range(n_col):
                if c * n_col + d < last:
                    z_copy(c * n_col + d).wait_recv()
                else:
                    for k in range(PARTS):
                        z_part(k).wait_recv()
        scale = scale_in[...]
        for k in range(TOK // 16):
            rows = slice(k * 16, (k + 1) * 16)
            x = zrecv[c, rows, :].astype(jnp.float32)
            inv = lax.rsqrt(jnp.mean(x * x, axis=-1, keepdims=True) + NORM_EPS)
            xbuf[rows, :] = (x * inv * scale).astype(jnp.bfloat16)

        def project(n, _):
            cols = pl.ds(pl.multiple_of(n * WIDE, WIDE), WIDE)
            x = xbuf[...]
            qbuf[:, cols] = jnp.dot(x, arena[0:width, cols], preferred_element_type=jnp.float32).astype(jnp.bfloat16)
            kbuf[c * TOK:(c + 1) * TOK, cols] = jnp.dot(x, arena[width:2 * width, cols], preferred_element_type=jnp.float32).astype(jnp.bfloat16)
            vbuf[c * TOK:(c + 1) * TOK, cols] = jnp.dot(x, arena[2 * width:3 * width, cols], preferred_element_type=jnp.float32).astype(jnp.bfloat16)
            return 0
        with jax.named_scope('project'):
            lax.fori_loop(0, halves, project, 0)
        hook(0)
        seen = (c + 1) * TOK
        q_at = lax.broadcasted_iota(jnp.int32, (TOK, seen), 0) + c * TOK
        k_at = lax.broadcasted_iota(jnp.int32, (TOK, seen), 1)
        causal = q_at >= k_at

        def head(h, _):
            cols = [pl.ds(pl.multiple_of((h * GROUP + u) * head_dim, head_dim), head_dim) for u in range(GROUP)]
            logits = [lax.dot_general(qbuf[:, at], kbuf[0:seen, at], (((1,), (1,)), ((), ())), preferred_element_type=jnp.float32) for at in cols]
            logits = [jnp.where(causal, s * (head_dim ** -0.5), -1e30) for s in logits]
            probs = [jnp.exp(s - jnp.max(s, axis=-1, keepdims=True)) for s in logits]
            sums = [jnp.sum(p, axis=-1, keepdims=True) for p in probs]
            mixed = [jnp.dot(p.astype(jnp.bfloat16), vbuf[0:seen, at], preferred_element_type=jnp.float32) for p, at in zip(probs, cols)]
            for at, m, t in zip(cols, mixed, sums):
                xbuf[:, at] = (m / t).astype(jnp.bfloat16)
            return 0
        with jax.named_scope('heads'):
            lax.fori_loop(0, heads // GROUP, head, 0)
        hook(1)

        def output(k, _):
            n = c * n_out + 2 * k
            cols = pl.ds(pl.multiple_of(2 * k * OUT, 2 * OUT), 2 * OUT)
            w_copy(n).wait()
            w_copy(n + 1).wait()
            w = jnp.concatenate([wo_buf[n % WSLOT], wo_buf[(n + 1) % WSLOT]], axis=1)
            proj = jnp.dot(xbuf[...], w, preferred_element_type=jnp.float32).astype(jnp.bfloat16)
            zrecv[c, :, cols] = (zrecv[c, :, cols].astype(jnp.float32) + proj.astype(jnp.float32)).astype(jnp.bfloat16)

            @pl.when(n + WSLOT < n_tok * n_out)
            def _():
                w_copy(n + WSLOT).start()
                w_copy(n + 1 + WSLOT).start()
            return 0
        with jax.named_scope('output'):
            lax.fori_loop(0, n_out // 2, output, 0)
        pltpu.make_async_copy(zrecv.at[c], out_hbm.at[c], out_sem.at[c]).start()
        hook(2)

    with jax.named_scope('relay'):
        relay(0)
        finish(6)
        relay(1)
        relay(2)
    finish(7)
    plan = {(0, 0): (8,), (0, 2): (9,), (1, 0): (10,), (1, 2): (11, 12), (2, 0): (13,), (2, 2): (14, 15)}
    for c in range(n_tok):
        def hook(at, c=c):
            for j in plan.get((c, at), ()):
                with jax.named_scope('fin'):
                    if j == last:
                        finish_last()
                    else:
                        finish(j)
        with jax.named_scope('attend'):
            attend(c, hook)

    def drain(i, _):
        y_copy(i).wait_send()
        z_copy(i).wait_send()
        return 0
    lax.fori_loop(0, last, drain, 0)
    for k in range(PARTS):
        y_part(k).wait_send()
        z_part(k).wait_send()
    for d in range(n_col):
        d_copy(d).wait_send()
    for r in range(3):
        for k in range(3):
            t_copy(k, r).wait_send()
    for c in range(n_tok):
        pltpu.make_async_copy(zrecv.at[c], out_hbm.at[c], out_sem.at[c]).wait()


def run_stage(pp_size, expert_out, ids, slot, gate, resid, scale, wq, wk, wv, wo):
    experts, cap_all, width = expert_out.shape
    tokens = resid.shape[0]
    heads = wq.shape[1]
    slots = experts * cap_all // 4
    n_tok, n_col = tokens // TOK, width // COL
    n_piece = n_tok * n_col
    dma = pltpu.SemaphoreType.DMA
    anyspace = pl.BlockSpec(memory_space=pl.ANY)
    vmem = pl.BlockSpec(memory_space=pltpu.VMEM)
    f32, bf16 = jnp.float32, jnp.bfloat16
    return pl.pallas_call(
        functools.partial(stage_kernel, pp_size, heads),
        out_shape=jax.ShapeDtypeStruct((n_tok, TOK, width), bf16),
        in_specs=[anyspace, vmem, vmem, vmem, anyspace, vmem, anyspace, anyspace, anyspace, anyspace],
        out_specs=anyspace,
        scratch_shapes=[
            pltpu.VMEM((max(4 * slots, 3 * width), width), bf16),
            pltpu.VMEM((3, 8, tokens), jnp.int32), pltpu.VMEM((3, 8, tokens), jnp.int32), pltpu.VMEM((3, 8, tokens), f32),
            pltpu.VMEM((tokens, 64), f32),
            pltpu.VMEM((3 * TOK, slots), bf16), pltpu.VMEM((3 * TOK, slots), bf16),
            pltpu.VMEM((n_piece, TOK, COL), f32), pltpu.VMEM((n_piece, TOK, COL), f32), pltpu.VMEM((n_piece, TOK, COL), f32),
            pltpu.VMEM((n_col, TOK, COL), f32), pltpu.VMEM((n_col, TOK, COL), f32),
            pltpu.VMEM((n_piece, TOK, COL), bf16),
            pltpu.VMEM((n_tok, TOK, width), bf16),
            pltpu.VMEM((STAGED, BLK, heads, width // heads), bf16),
            pltpu.VMEM((WSLOT, width, OUT), bf16),
            pltpu.VMEM((TOK, width), bf16), pltpu.VMEM((tokens, width), bf16), pltpu.VMEM((tokens, width), bf16), pltpu.VMEM((TOK, width), bf16),
            dma((4,)), dma((n_piece,)), dma((3, 3)), dma((3, 3)), dma((n_col,)), dma((n_col,)),
            pltpu.SemaphoreType.REGULAR,
            dma((n_piece,)), dma((n_piece,)), dma((n_piece,)), dma((n_piece,)), dma((PARTS,)), dma((PARTS,)), dma((PARTS,)), dma((PARTS,)), dma((STAGED,)), dma((WSLOT,)), dma((n_tok,)),
        ],
        compiler_params=pltpu.CompilerParams(collective_id=0, has_side_effects=True, vmem_limit_bytes=67043328),
    )(expert_out, ids, slot, gate, resid, scale, wq, wk, wv, wo)


def solution(mesh):
    pp_size = mesh.shape['pp']
    token_spec = P(('data', 'pp'), 'ep', None, None)
    weight_spec = P('pp', None, None, None)

    def body(expert_out, expert_ids, slot_ids, gate_vals, residual, norm_scale, w_query, w_key, w_value, w_out):
        ids, slot, gate = (jnp.swapaxes(a[0, 0], 0, 1) for a in (expert_ids, slot_ids, gate_vals))
        width = expert_out.shape[-1]
        result = run_stage(pp_size, expert_out[0], ids, slot, gate, residual[0, 0], norm_scale, w_query[0], w_key[0], w_value[0], w_out[0].reshape(-1, width))
        return result.reshape(residual.shape)

    return jax.shard_map(body, mesh=mesh, in_specs=(token_spec, token_spec, token_spec, token_spec, token_spec, P('pp', None), weight_spec, weight_spec, weight_spec, weight_spec), out_specs=token_spec, check_vma=False)
```

```python
import functools

import jax
import jax.numpy as jnp
from jax import lax
from jax.experimental import pallas as pl
from jax.experimental.pallas import tpu as pltpu
from jax.sharding import PartitionSpec as P

NORM_EPS = 1e-6
MESH = pl.DeviceIdType.MESH
TOK = 128
COL = 512
WIDE = 1024
BLK = 128
GROUP = 16
PARTS = 4


def stage_kernel(pp_size, heads, o_hbm, ids_in, slot_in, gate_in, h_hbm, scale_in, wq_hbm, wk_hbm, wv_hbm, wo_hbm, out_hbm,
                 arena, mine, theirs, tblt, gate_a, gate_b, ysend, acc, yrecv, dsend, drecv, hz, zrecv, panel, qbuf, kbuf, vbuf, xbuf,
                 o_sem, h_sem, t_ssem, t_rsem, d_ssem, d_rsem, credit, y_ssem, y_rsem, z_ssem, z_rsem, yp_ssem, yp_rsem, zp_ssem, zp_rsem, s_sem, out_sem):
    experts, cap_all, width = o_hbm.shape
    cap = cap_all // 4
    slots = experts * cap
    tokens = h_hbm.shape[0]
    head_dim = width // heads
    n_tok, n_col = tokens // TOK, width // COL
    n_piece = n_tok * n_col
    gates = (gate_b, gate_a)
    me = lax.axis_index('ep')
    core = lax.rem(me, 2)
    row = me // 2
    partner = row * 2 + (1 - core)
    peer = (1 - row) * 2 + core
    diag = (1 - row) * 2 + (1 - core)
    owners = (diag, peer, partner, me)
    stage = lax.axis_index('pp')
    nxt = lax.rem(stage + 1, pp_size)
    prv = lax.rem(stage + pp_size - 1, pp_size)

    def o_start(r):
        def one(e, _):
            pltpu.make_async_copy(o_hbm.at[e, pl.ds(owners[r] * cap, cap)],
                                  arena.at[pl.ds(pl.multiple_of(r * slots + e * cap, 16), cap)], o_sem.at[r]).start()
            return 0
        lax.fori_loop(0, experts, one, 0)

    def o_wait(r):
        view = arena.at[pl.ds(r * slots, slots)]
        pltpu.make_async_copy(view, view, o_sem.at[r]).wait()

    def h_copy(i):
        c, d = i // n_col, i % n_col
        return pltpu.make_async_copy(h_hbm.at[pl.ds(c * TOK, TOK), pl.ds(d * COL, COL)], hz.at[i], h_sem.at[i])

    def t_copy(r):
        return pltpu.make_async_remote_copy(src_ref=mine, dst_ref=theirs.at[r], send_sem=t_ssem.at[r], recv_sem=t_rsem.at[r],
                                            device_id={'ep': owners[r]}, device_id_type=MESH)

    def d_copy(d):
        return pltpu.make_async_remote_copy(src_ref=dsend.at[d], dst_ref=drecv.at[d], send_sem=d_ssem.at[d],
                                            recv_sem=d_rsem.at[d], device_id={'ep': partner}, device_id_type=MESH)

    def y_copy(i):
        return pltpu.make_async_remote_copy(src_ref=ysend.at[i], dst_ref=yrecv.at[i], send_sem=y_ssem.at[i], recv_sem=y_rsem.at[i],
                                            device_id={'ep': peer}, device_id_type=MESH)

    def z_copy(i):
        c, d = i // n_col, i % n_col
        return pltpu.make_async_remote_copy(src_ref=hz.at[i], dst_ref=zrecv.at[c, :, pl.ds(pl.multiple_of(d * COL, COL), COL)],
                                            send_sem=z_ssem.at[i], recv_sem=z_rsem.at[i], device_id={'pp': nxt}, device_id_type=MESH)

    last = n_piece - 1
    thin = TOK // PARTS

    def y_part(k):
        rows = pl.ds(k * thin, thin)
        return pltpu.make_async_remote_copy(src_ref=ysend.at[last, rows], dst_ref=yrecv.at[last, rows], send_sem=yp_ssem.at[k],
                                            recv_sem=yp_rsem.at[k], device_id={'ep': peer}, device_id_type=MESH)

    def z_part(k):
        rows = pl.ds(k * thin, thin)
        return pltpu.make_async_remote_copy(src_ref=hz.at[last, rows], dst_ref=zrecv.at[n_tok - 1, rows, pl.ds(width - COL, COL)],
                                            send_sem=zp_ssem.at[k], recv_sem=zp_rsem.at[k], device_id={'pp': nxt}, device_id_type=MESH)

    raw = (wq_hbm, wk_hbm, wv_hbm)

    n_blk = width // BLK
    rows_blk = BLK * heads

    def s_copy(w, b):
        return pltpu.make_async_copy(raw[w].at[pl.ds(b * rows_blk, rows_blk)], panel.at[b], s_sem.at[b])

    def w_copy(q):
        return pltpu.make_async_copy(wo_hbm.at[:, pl.ds(q * head_dim, head_dim)], panel.at[q], s_sem.at[q])

    lane_row = lax.broadcasted_iota(jnp.int32, (16, tokens), 0)

    def keyed(r, table):
        shift = jnp.where(lane_row < 8, me * slots, 0).astype(jnp.float32)
        tblt[:, r * 16:(r + 1) * 16] = jnp.transpose(table - shift)

    groups = TOK // 16

    def build(c, r, q):
        t = tblt[pl.ds(pl.multiple_of(c * TOK + q * 16, 16), 16), r * 16:(r + 1) * 16]
        lane = lax.broadcasted_iota(jnp.int32, (16, slots), 1).astype(jnp.float32)
        g = jnp.zeros((16, slots), jnp.float32)
        for j in range(8):
            g = jnp.where(lane == t[:, j:j + 1], t[:, 8 + j:9 + j], g)
        g1 = g.astype(jnp.bfloat16)
        rest = g - g1.astype(jnp.float32)
        g2 = rest.astype(jnp.bfloat16)
        g3 = (rest - g2.astype(jnp.float32)).astype(jnp.bfloat16)
        at = pl.multiple_of(q * 16, 16)
        dst = gates[r % 2]
        dst[pl.ds(at, 16), :] = g1
        dst[pl.ds(at + TOK, 16), :] = g2
        dst[pl.ds(at + 2 * TOK, 16), :] = g3

    halves = width // WIDE

    def dot_role(r, h, per):
        w = arena[r * slots:(r + 1) * slots, h * COL:(h + per) * COL]
        p = jnp.dot(gates[r % 2][...], w, preferred_element_type=jnp.float32)
        total = p[:TOK] + p[TOK:2 * TOK] + p[2 * TOK:]
        return [(h + u, total[:, u * COL:(u + 1) * COL]) for u in range(per)]

    def build_now(c, r):
        for q in range(groups):
            build(c, r, q)

    def give():
        pl.semaphore_signal(credit, inc=1, device_id={'ep': partner}, device_id_type=MESH)

    def hold(d):
        d_copy(d).wait_send()
        pl.semaphore_wait(credit, 1)

    def finish(j):
        y_copy(j).wait_recv()
        hz[j] = (acc[j] + yrecv[j]).astype(jnp.bfloat16)
        z_copy(j).start()

    def finish_last():
        for k in range(PARTS):
            rows = pl.ds(k * thin, thin)
            y_part(k).wait_recv()
            hz[last, rows] = (acc[last, rows] + yrecv[last, rows]).astype(jnp.bfloat16)
            z_part(k).start()

    o_start(0)
    barrier = pltpu.get_barrier_semaphore()
    for dev in (partner, peer, diag):
        pl.semaphore_signal(barrier, inc=1, device_id={'ep': dev}, device_id_type=MESH)
    for dev in (nxt, prv):
        pl.semaphore_signal(barrier, inc=1, device_id={'pp': dev}, device_id_type=MESH)
    slot = slot_in[...]
    mine[0:8] = jnp.where(slot >= 0, ids_in[...] * cap + (slot - me * cap), -1).astype(jnp.float32)
    mine[8:16] = gate_in[...]
    pl.semaphore_wait(barrier, 5)
    for r in range(3):
        t_copy(r).start()
    o_start(1)
    keyed(3, mine[...])
    for i in range(n_col):
        h_copy(i).start()
    for r in range(3):
        t_copy(r).wait_recv()
        keyed(r, theirs[r])
        if r == 0:
            build_now(0, 0)
    o_start(2)
    o_start(3)

    def rest_h(i, _):
        h_copy(i).start()
        return 0
    lax.fori_loop(n_col, n_piece, rest_h, 0)

    def at_first(c, r):
        @pl.when(c == 0)
        def _():
            o_wait(r)

    def chunk(c, _):
        @pl.when(c == 1)
        def _():
            for q in range(n_blk):
                s_copy(0, q).start()

        def fill(d):
            i = c * n_col + d
            d_copy(d).wait_recv()
            ysend[i] += drecv[d]
            give()
            if d < n_col - 1:
                y_copy(i).start()
            else:
                @pl.when(c < n_tok - 1)
                def _():
                    y_copy(i).start()

                @pl.when(c == n_tok - 1)
                def _():
                    for k in range(PARTS):
                        y_part(k).start()

        def out_role(r, h, per, ahead=None):
            for d in range(h, h + per):
                if r == 0:
                    @pl.when(c > 0)
                    def _():
                        hold(d)
                else:
                    hold(d)
            if h == 0:
                at_first(c, r)
            for d, value in dot_role(r, h, per):
                dsend[d] = value
            if ahead is not None:
                build_now(*ahead)
            for d in range(h, h + per):
                d_copy(d).start()

        def near_role(h, per, ahead=None):
            if h == 0:
                at_first(c, 1)
            for d, value in dot_role(1, h, per):
                ysend[c * n_col + d] = value
            if ahead is not None:
                build_now(*ahead)
            for d in range(h, h + per):
                fill(d)

        def own_role(h, per, ahead=None):
            for d in range(h, h + per):
                h_copy(c * n_col + d).wait()
            if h == 0:
                at_first(c, 3)
            for d, value in dot_role(3, h, per):
                i = c * n_col + d
                acc[i] = value + hz[i].astype(jnp.float32)
            if ahead is not None:
                build_now(*ahead)
            for d in range(h, h + per):
                d_copy(d).wait_recv()
                acc[c * n_col + d] += drecv[d]

                @pl.when(c < n_tok - 1)
                def _():
                    give()

        half = n_col // 2
        out_role(0, 0, 1, (c, 1))
        for d in range(1, half):
            out_role(0, d, 1)
        for d in range(half):
            near_role(d, 1)
        out_role(0, half, half)
        near_role(half, half, (c, 2))
        out_role(2, 0, half, (c, 3))
        out_role(2, half, half)
        own_role(0, half)
        own_role(half, half, (lax.rem(c + 1, n_tok), 0))

        @pl.when(c > 0)
        def _():
            finish(2 * c - 2)
            finish(2 * c - 1)
        return 0

    with jax.named_scope('combine'):
        lax.fori_loop(0, n_tok, chunk, 0)

    def relay(w):
        def block(b, _):
            s_copy(w, b).wait()
            for k in range(BLK // 64):
                rows = panel[b, k * 64 * heads:(k + 1) * 64 * heads, :].reshape(64, heads, head_dim).reshape(64, width)
                arena[pl.ds(pl.multiple_of(w * width + b * BLK + k * 64, 64), 64), :] = rows
            if w < 2:
                s_copy(w + 1, b).start()
            else:
                w_copy(b).start()
            return 0
        lax.fori_loop(0, n_blk, block, 0)

    def out_copy(c, k):
        cols = pl.ds(k * WIDE, WIDE)
        return pltpu.make_async_copy(zrecv.at[c, :, cols], out_hbm.at[c, :, cols], out_sem.at[c, k])

    def attend(c, hook):
        with jax.named_scope('zwait'):
            for d in range(n_col):
                if c * n_col + d < last:
                    z_copy(c * n_col + d).wait_recv()
                else:
                    for k in range(PARTS):
                        z_part(k).wait_recv()
        scale = scale_in[...]
        for k in range(TOK // 16):
            rows = slice(k * 16, (k + 1) * 16)
            x = zrecv[c, rows, :].astype(jnp.float32)
            inv = lax.rsqrt(jnp.mean(x * x, axis=-1, keepdims=True) + NORM_EPS)
            xbuf[rows, :] = (x * inv * scale).astype(jnp.bfloat16)

        def project(n, _):
            cols = pl.ds(pl.multiple_of(n * WIDE, WIDE), WIDE)
            x = xbuf[...]
            qbuf[:, cols] = jnp.dot(x, arena[0:width, cols], preferred_element_type=jnp.float32).astype(jnp.bfloat16)
            kbuf[c * TOK:(c + 1) * TOK, cols] = jnp.dot(x, arena[width:2 * width, cols], preferred_element_type=jnp.float32).astype(jnp.bfloat16)
            vbuf[c * TOK:(c + 1) * TOK, cols] = jnp.dot(x, arena[2 * width:3 * width, cols], preferred_element_type=jnp.float32).astype(jnp.bfloat16)
            return 0
        with jax.named_scope('project'):
            lax.fori_loop(0, halves, project, 0)
        hook(0)
        seen = (c + 1) * TOK
        q_at = lax.broadcasted_iota(jnp.int32, (TOK, seen), 0) + c * TOK
        k_at = lax.broadcasted_iota(jnp.int32, (TOK, seen), 1)
        causal = q_at >= k_at

        def head(h, _):
            cols = [pl.ds(pl.multiple_of((h * GROUP + u) * head_dim, head_dim), head_dim) for u in range(GROUP)]
            logits = [lax.dot_general(qbuf[:, at], kbuf[0:seen, at], (((1,), (1,)), ((), ())), preferred_element_type=jnp.float32) for at in cols]
            logits = [jnp.where(causal, s * (head_dim ** -0.5), -1e30) for s in logits]
            probs = [jnp.exp(s - jnp.max(s, axis=-1, keepdims=True)) for s in logits]
            sums = [jnp.sum(p, axis=-1, keepdims=True) for p in probs]
            mixed = [jnp.dot(p.astype(jnp.bfloat16), vbuf[0:seen, at], preferred_element_type=jnp.float32) for p, at in zip(probs, cols)]
            for at, m, t in zip(cols, mixed, sums):
                xbuf[:, at] = (m / t).astype(jnp.bfloat16)
            return 0
        with jax.named_scope('heads'):
            lax.fori_loop(0, heads // GROUP, head, 0)
        hook(1)

        if c == 0:
            for q in range(heads):
                w_copy(q).wait()
        with jax.named_scope('output'):
            for k in range(halves):
                cols = slice(k * WIDE, (k + 1) * WIDE)
                w = jnp.concatenate([panel[q] for q in range(k * WIDE // head_dim, (k + 1) * WIDE // head_dim)], axis=1)
                proj = jnp.dot(xbuf[...], w, preferred_element_type=jnp.float32).astype(jnp.bfloat16)
                zrecv[c, :, cols] = (zrecv[c, :, cols].astype(jnp.float32) + proj.astype(jnp.float32)).astype(jnp.bfloat16)
                out_copy(c, k).start()
        hook(2)

    finish(6)
    with jax.named_scope('relay'):
        relay(0)
        relay(1)
        finish(7)
        relay(2)
    finish(8)
    plan = {(0, 2): (9,), (1, 2): (10, 11), (2, 0): (12,), (2, 1): (13,), (2, 2): (14, 15)}
    for c in range(n_tok):
        def hook(at, c=c):
            for j in plan.get((c, at), ()):
                with jax.named_scope('fin'):
                    if j == last:
                        finish_last()
                    else:
                        finish(j)
        with jax.named_scope('attend'):
            attend(c, hook)

    def drain(i, _):
        y_copy(i).wait_send()
        z_copy(i).wait_send()
        return 0
    lax.fori_loop(0, last, drain, 0)
    for k in range(PARTS):
        y_part(k).wait_send()
        z_part(k).wait_send()
    for d in range(n_col):
        d_copy(d).wait_send()
    for r in range(3):
        t_copy(r).wait_send()
    for c in range(n_tok):
        for k in range(halves):
            out_copy(c, k).wait()


def copy_kernel(src, dst, hold, in_sem, out_sem):
    steps = src.shape[0]
    for c in range(steps):
        pltpu.make_async_copy(src.at[c], hold.at[c], in_sem.at[c]).start()
    for c in range(steps):
        pltpu.make_async_copy(src.at[c], hold.at[c], in_sem.at[c]).wait()
        pltpu.make_async_copy(hold.at[c], dst.at[c], out_sem.at[c]).start()
    for c in range(steps):
        pltpu.make_async_copy(hold.at[c], dst.at[c], out_sem.at[c]).wait()


def settle(x):
    anyspace = pl.BlockSpec(memory_space=pl.ANY)
    dma = pltpu.SemaphoreType.DMA
    return pl.pallas_call(copy_kernel, out_shape=jax.ShapeDtypeStruct(x.shape, x.dtype), in_specs=[anyspace], out_specs=anyspace,
                          scratch_shapes=[pltpu.VMEM(x.shape, x.dtype), dma((x.shape[0],)), dma((x.shape[0],))])(x)


def run_stage(pp_size, heads, expert_out, ids, slot, gate, resid, scale, wq, wk, wv, wo):
    experts, cap_all, width = expert_out.shape
    tokens = resid.shape[0]
    slots = experts * cap_all // 4
    n_tok, n_col = tokens // TOK, width // COL
    n_piece = n_tok * n_col
    dma = pltpu.SemaphoreType.DMA
    anyspace = pl.BlockSpec(memory_space=pl.ANY)
    vmem = pl.BlockSpec(memory_space=pltpu.VMEM)
    f32, bf16 = jnp.float32, jnp.bfloat16
    return pl.pallas_call(
        functools.partial(stage_kernel, pp_size, heads),
        out_shape=jax.ShapeDtypeStruct((n_tok, TOK, width), bf16),
        in_specs=[anyspace, vmem, vmem, vmem, anyspace, vmem, anyspace, anyspace, anyspace, anyspace],
        out_specs=anyspace,
        scratch_shapes=[
            pltpu.VMEM((max(4 * slots, 3 * width), width), bf16),
            pltpu.VMEM((16, tokens), f32), pltpu.VMEM((3, 16, tokens), f32),
            pltpu.VMEM((tokens, 64), f32),
            pltpu.VMEM((3 * TOK, slots), bf16), pltpu.VMEM((3 * TOK, slots), bf16),
            pltpu.VMEM((n_piece, TOK, COL), f32), pltpu.VMEM((n_piece, TOK, COL), f32), pltpu.VMEM((n_piece, TOK, COL), f32),
            pltpu.VMEM((n_col, TOK, COL), f32), pltpu.VMEM((n_col, TOK, COL), f32),
            pltpu.VMEM((n_piece, TOK, COL), bf16),
            pltpu.VMEM((n_tok, TOK, width), bf16),
            pltpu.VMEM((width // BLK, width, width // heads), bf16),
            pltpu.VMEM((TOK, width), bf16), pltpu.VMEM((tokens, width), bf16), pltpu.VMEM((tokens, width), bf16), pltpu.VMEM((TOK, width), bf16),
            dma((4,)), dma((n_piece,)), dma((3,)), dma((3,)), dma((n_col,)), dma((n_col,)),
            pltpu.SemaphoreType.REGULAR,
            dma((n_piece,)), dma((n_piece,)), dma((n_piece,)), dma((n_piece,)), dma((PARTS,)), dma((PARTS,)), dma((PARTS,)), dma((PARTS,)), dma((width // BLK,)), dma((n_tok, width // WIDE)),
        ],
        compiler_params=pltpu.CompilerParams(collective_id=0, has_side_effects=True, vmem_limit_bytes=67043328),
    )(expert_out, ids, slot, gate, resid, scale, wq, wk, wv, wo)


def solution(mesh):
    pp_size = mesh.shape['pp']
    token_spec = P(('data', 'pp'), 'ep', None, None)
    weight_spec = P('pp', None, None, None)

    def body(expert_out, expert_ids, slot_ids, gate_vals, residual, norm_scale, w_query, w_key, w_value, w_out):
        ids, slot, gate = (jnp.swapaxes(a[0, 0], 0, 1) for a in (expert_ids, slot_ids, gate_vals))
        result = run_stage(pp_size, w_query.shape[2], expert_out[0], ids, slot, gate, residual[0, 0], norm_scale,
                           *(w[0].reshape(-1, w.shape[-1]) for w in (w_query, w_key, w_value, w_out)))
        return settle(result).reshape(residual.shape)

    return jax.shard_map(body, mesh=mesh, in_specs=(token_spec, token_spec, token_spec, token_spec, token_spec, P('pp', None), weight_spec, weight_spec, weight_spec, weight_spec), out_specs=token_spec, check_vma=False)
```

```python
import functools

import jax
import jax.numpy as jnp
from jax import lax
from jax.experimental import pallas as pl
from jax.experimental.pallas import tpu as pltpu
from jax.sharding import PartitionSpec as P

NORM_EPS = 1e-6
MESH = pl.DeviceIdType.MESH
TOK = 128
COL = 512
WIDE = 1024
BLK = 128
PARTS = 8


def stage_kernel(pp_size, heads, o_hbm, ids_in, slot_in, gate_in, h_hbm, scale_in, wq_hbm, wk_hbm, wv_hbm, wo_hbm, out_hbm,
                 arena, mine, theirs, tblt, gate_a, gate_b, ysend, acc, yrecv, dsend, drecv, hz, zrecv, panel, qbuf, kbuf, vbuf, xbuf, abuf,
                 o_sem, h_sem, t_ssem, t_rsem, d_ssem, d_rsem, credit, y_ssem, y_rsem, z_ssem, z_rsem, yp_rsem, s_sem, out_sem):
    experts, cap_all, width = o_hbm.shape
    cap = cap_all // 4
    slots = experts * cap
    tokens = h_hbm.shape[0]
    head_dim = width // heads
    n_tok, n_col = tokens // TOK, width // COL
    n_piece = n_tok * n_col
    gates = (gate_b, gate_a)
    me = lax.axis_index('ep')
    core = lax.rem(me, 2)
    row = me // 2
    partner = row * 2 + (1 - core)
    peer = (1 - row) * 2 + core
    diag = (1 - row) * 2 + (1 - core)
    owners = (diag, peer, partner, me)
    stage = lax.axis_index('pp')
    nxt = lax.rem(stage + 1, pp_size)
    prv = lax.rem(stage + pp_size - 1, pp_size)

    def o_start(r):
        def one(e, _):
            pltpu.make_async_copy(o_hbm.at[e, pl.ds(owners[r] * cap, cap)],
                                  arena.at[pl.ds(pl.multiple_of(r * slots + e * cap, 16), cap)], o_sem.at[r]).start()
            return 0
        lax.fori_loop(0, experts, one, 0)

    def o_wait(r):
        view = arena.at[pl.ds(r * slots, slots)]
        pltpu.make_async_copy(view, view, o_sem.at[r]).wait()

    def h_copy(i):
        c, d = i // n_col, i % n_col
        return pltpu.make_async_copy(h_hbm.at[pl.ds(c * TOK, TOK), pl.ds(d * COL, COL)], hz.at[i], h_sem.at[c])

    cuts = (pl.ds(0, TOK), pl.ds(TOK, tokens - TOK))

    def t_copy(r, part):
        at = cuts[part]
        return pltpu.make_async_remote_copy(src_ref=mine.at[:, at], dst_ref=theirs.at[r, :, at], send_sem=t_ssem.at[part, r],
                                            recv_sem=t_rsem.at[part, r], device_id={'ep': owners[r]}, device_id_type=MESH)

    def d_copy(d):
        return pltpu.make_async_remote_copy(src_ref=dsend.at[d], dst_ref=drecv.at[d], send_sem=d_ssem.at[d],
                                            recv_sem=d_rsem.at[d], device_id={'ep': partner}, device_id_type=MESH)

    def y_copy(i):
        return pltpu.make_async_remote_copy(src_ref=ysend.at[i], dst_ref=yrecv.at[i], send_sem=y_ssem, recv_sem=y_rsem.at[i],
                                            device_id={'ep': peer}, device_id_type=MESH)

    def z_copy(i):
        c, d = i // n_col, i % n_col
        return pltpu.make_async_remote_copy(src_ref=hz.at[i], dst_ref=zrecv.at[c, :, pl.ds(pl.multiple_of(d * COL, COL), COL)],
                                            send_sem=z_ssem, recv_sem=z_rsem.at[c], device_id={'pp': nxt}, device_id_type=MESH)

    y_all = pltpu.make_async_remote_copy(src_ref=ysend, dst_ref=ysend, send_sem=y_ssem, recv_sem=y_rsem.at[0],
                                         device_id={'ep': peer}, device_id_type=MESH)
    z_all = pltpu.make_async_remote_copy(src_ref=hz, dst_ref=hz, send_sem=z_ssem, recv_sem=z_rsem.at[0],
                                         device_id={'pp': nxt}, device_id_type=MESH)
    last = n_piece - 1
    thin = TOK // PARTS

    def y_part(k):
        rows = pl.ds(k * thin, thin)
        return pltpu.make_async_remote_copy(src_ref=ysend.at[last, rows], dst_ref=yrecv.at[last, rows], send_sem=y_ssem,
                                            recv_sem=yp_rsem.at[k], device_id={'ep': peer}, device_id_type=MESH)

    def z_part(k):
        rows = pl.ds(k * thin, thin)
        return pltpu.make_async_remote_copy(src_ref=hz.at[last, rows], dst_ref=zrecv.at[n_tok - 1, rows, pl.ds(width - COL, COL)],
                                            send_sem=z_ssem, recv_sem=z_rsem.at[n_tok - 1], device_id={'pp': nxt}, device_id_type=MESH)

    raw = (wq_hbm, wk_hbm, wv_hbm)

    n_blk = width // BLK
    rows_blk = BLK * heads

    def s_copy(w, b):
        return pltpu.make_async_copy(raw[w].at[pl.ds(b * rows_blk, rows_blk)], panel.at[b], s_sem.at[b])

    def w_copy(q):
        return pltpu.make_async_copy(wo_hbm.at[:, pl.ds(q * head_dim, head_dim)], panel.at[q], s_sem.at[q])

    def keyed(r, table, part):
        lane_row = lax.broadcasted_iota(jnp.int32, table.shape, 0)
        shift = jnp.where(lane_row < 8, me * slots, 0).astype(jnp.float32)
        tblt[cuts[part], r * 16:(r + 1) * 16] = jnp.transpose(table - shift)

    groups = TOK // 16

    def build(c, r, q):
        t = tblt[pl.ds(pl.multiple_of(c * TOK + q * 16, 16), 16), r * 16:(r + 1) * 16]
        lane = lax.broadcasted_iota(jnp.int32, (16, slots), 1).astype(jnp.float32)
        g = jnp.zeros((16, slots), jnp.float32)
        for j in range(8):
            g = jnp.where(lane == t[:, j:j + 1], t[:, 8 + j:9 + j], g)
        g1 = g.astype(jnp.bfloat16)
        rest = g - g1.astype(jnp.float32)
        g2 = rest.astype(jnp.bfloat16)
        g3 = (rest - g2.astype(jnp.float32)).astype(jnp.bfloat16)
        at = pl.multiple_of(q * 16, 16)
        dst = gates[r % 2]
        dst[pl.ds(at, 16), :] = g1
        dst[pl.ds(at + TOK, 16), :] = g2
        dst[pl.ds(at + 2 * TOK, 16), :] = g3

    halves = width // WIDE

    def dot_role(r, h, per):
        w = arena[r * slots:(r + 1) * slots, h * COL:(h + per) * COL]
        p = jnp.dot(gates[r % 2][...], w, preferred_element_type=jnp.float32)
        total = p[:TOK] + p[TOK:2 * TOK] + p[2 * TOK:]
        return [(h + u, total[:, u * COL:(u + 1) * COL]) for u in range(per)]

    def build_now(c, r):
        for q in range(groups):
            build(c, r, q)

    def give():
        pl.semaphore_signal(credit, inc=1, device_id={'ep': partner}, device_id_type=MESH)

    def hold(d):
        d_copy(d).wait_send()
        pl.semaphore_wait(credit, 1)

    def finish(j):
        y_copy(j).wait_recv()
        hz[j] = (acc[j] + yrecv[j]).astype(jnp.bfloat16)
        z_copy(j).start()

    def finish_last():
        for k in range(PARTS):
            rows = pl.ds(k * thin, thin)
            y_part(k).wait_recv()
            hz[last, rows] = (acc[last, rows] + yrecv[last, rows]).astype(jnp.bfloat16)
            z_part(k).start()

    barrier = pltpu.get_barrier_semaphore()
    for dev in (partner, peer, diag):
        pl.semaphore_signal(barrier, inc=1, device_id={'ep': dev}, device_id_type=MESH)
    for dev in (nxt, prv):
        pl.semaphore_signal(barrier, inc=1, device_id={'pp': dev}, device_id_type=MESH)
    slot = slot_in[...]
    mine[0:8] = jnp.where(slot >= 0, ids_in[...] * cap + (slot - me * cap), -1).astype(jnp.float32)
    mine[8:16] = gate_in[...]
    o_start(0)
    pl.semaphore_wait(barrier, 5)
    for part in range(2):
        for r in range(3):
            t_copy(r, part).start()
    o_start(1)
    for part in range(2):
        keyed(3, mine[:, cuts[part]], part)

    def table(r, part):
        t_copy(r, part).wait_recv()
        keyed(r, theirs[r, :, cuts[part]], part)

    table(0, 0)
    build_now(0, 0)
    table(1, 0)

    def later():
        o_start(2)
        o_start(3)

        def one(i, _):
            h_copy(i).start()
            return 0
        lax.fori_loop(0, n_piece, one, 0)
        table(2, 0)
        for r in range(3):
            table(r, 1)

    def at_first(c, r):
        @pl.when(c == 0)
        def _():
            o_wait(r)

    def chunk(c, _):
        @pl.when(c == 1)
        def _():
            for q in range(n_blk):
                s_copy(0, q).start()

        def fill(d):
            i = c * n_col + d
            d_copy(d).wait_recv()
            ysend[i] += drecv[d]
            give()
            if d < n_col - 1:
                y_copy(i).start()
            else:
                @pl.when(c < n_tok - 1)
                def _():
                    y_copy(i).start()

                @pl.when(c == n_tok - 1)
                def _():
                    for k in range(PARTS):
                        y_part(k).start()

        def out_role(r, h, per, ahead=None):
            for d in range(h, h + per):
                if r == 0:
                    @pl.when(c > 0)
                    def _():
                        hold(d)
                else:
                    hold(d)
            if h == 0:
                at_first(c, r)
            for d, value in dot_role(r, h, per):
                dsend[d] = value
            if ahead is not None:
                build_now(*ahead)
            for d in range(h, h + per):
                d_copy(d).start()

        def near_role(h, per, ahead=None):
            if h == 0:
                at_first(c, 1)
            for d, value in dot_role(1, h, per):
                ysend[c * n_col + d] = value
            if ahead is not None:
                build_now(*ahead)
            for d in range(h, h + per):
                fill(d)

        def own_role(h, per, ahead=None):
            if h == 0:
                view = hz.at[pl.ds(c * n_col, n_col)]
                pltpu.make_async_copy(view, view, h_sem.at[c]).wait()
                at_first(c, 3)
            for d, value in dot_role(3, h, per):
                i = c * n_col + d
                acc[i] = value + hz[i].astype(jnp.float32)
            if ahead is not None:
                build_now(*ahead)
            for d in range(h, h + per):
                d_copy(d).wait_recv()
                acc[c * n_col + d] += drecv[d]

                @pl.when(c < n_tok - 1)
                def _():
                    give()

        half = n_col // 2
        out_role(0, 0, 1, (c, 1))

        for d in range(1, half):
            out_role(0, d, 1)
        for d in range(half):
            near_role(d, 1)
            if d == 0:
                pl.when(c == 0)(later)
        out_role(0, half, half)
        near_role(half, half, (c, 2))
        out_role(2, 0, half, (c, 3))
        out_role(2, half, half)
        own_role(0, half)
        own_role(half, half, (lax.rem(c + 1, n_tok), 0))

        @pl.when(c > 0)
        def _():
            finish(2 * c - 2)
            finish(2 * c - 1)
        return 0

    with jax.named_scope('combine'):
        lax.fori_loop(0, n_tok, chunk, 0)

    def relay(w):
        def block(b, _):
            s_copy(w, b).wait()
            for k in range(BLK // 64):
                rows = panel[b, k * 64 * heads:(k + 1) * 64 * heads, :].reshape(64, heads, head_dim).reshape(64, width)
                arena[pl.ds(pl.multiple_of(w * width + b * BLK + k * 64, 64), 64), :] = rows
            if w < 2:
                s_copy(w + 1, b).start()
            else:
                w_copy(b).start()
            return 0
        lax.fori_loop(0, n_blk, block, 0)

    def out_copy(c, k):
        cols = pl.ds(k * WIDE, WIDE)
        return pltpu.make_async_copy(zrecv.at[c, :, cols], out_hbm.at[c, :, cols], out_sem)

    def attend(c, hook):
        with jax.named_scope('zwait'):
            pltpu.make_async_copy(zrecv.at[c], zrecv.at[c], z_rsem.at[c]).wait()
        scale = scale_in[...]
        for k in range(TOK // 16):
            rows = slice(k * 16, (k + 1) * 16)
            x = zrecv[c, rows, :].astype(jnp.float32)
            inv = lax.rsqrt(jnp.mean(x * x, axis=-1, keepdims=True) + NORM_EPS)
            xbuf[rows, :] = (x * inv * scale).astype(jnp.bfloat16)

        seen = (c + 1) * TOK
        q_at = lax.broadcasted_iota(jnp.int32, (TOK, seen), 0) + c * TOK
        k_at = lax.broadcasted_iota(jnp.int32, (TOK, seen), 1)
        causal = q_at >= k_at

        def project(n, wide):
            cols = pl.ds(n, wide)
            x = xbuf[...]
            qbuf[:, cols] = jnp.dot(x, arena[0:width, cols], preferred_element_type=jnp.float32).astype(jnp.bfloat16)
            kbuf[c * TOK:(c + 1) * TOK, cols] = jnp.dot(x, arena[width:2 * width, cols], preferred_element_type=jnp.float32).astype(jnp.bfloat16)
            vbuf[c * TOK:(c + 1) * TOK, cols] = jnp.dot(x, arena[2 * width:3 * width, cols], preferred_element_type=jnp.float32).astype(jnp.bfloat16)

        def mix(first, count):
            cols = [pl.ds((first + u) * head_dim, head_dim) for u in range(count)]
            logits = [lax.dot_general(qbuf[:, at], kbuf[0:seen, at], (((1,), (1,)), ((), ())), preferred_element_type=jnp.float32) for at in cols]
            logits = [jnp.where(causal, s * (head_dim ** -0.5), -1e30) for s in logits]
            probs = [jnp.exp(s - jnp.max(s, axis=-1, keepdims=True)) for s in logits]
            sums = [jnp.sum(p, axis=-1, keepdims=True) for p in probs]
            mixed = [jnp.dot(p.astype(jnp.bfloat16), vbuf[0:seen, at], preferred_element_type=jnp.float32) for p, at in zip(probs, cols)]
            for at, m, t in zip(cols, mixed, sums):
                abuf[:, at] = (m / t).astype(jnp.bfloat16)

        if c == n_tok - 1:
            with jax.named_scope('lastmix'):
                for k in range(halves):
                    project(k * WIDE, WIDE)
                    mix(k * heads // halves, heads // halves)
        else:
            def one(n, _):
                project(pl.multiple_of(n * WIDE, WIDE), WIDE)
                return 0
            with jax.named_scope('project'):
                lax.fori_loop(0, halves, one, 0)
            hook(0)
            with jax.named_scope('heads'):
                mix(0, heads)
            hook(1)
        if c == 0:
            for q in range(heads):
                w_copy(q).wait()
        with jax.named_scope('output'):
            for k in range(halves):
                cols = slice(k * WIDE, (k + 1) * WIDE)
                w = jnp.concatenate([panel[q] for q in range(k * WIDE // head_dim, (k + 1) * WIDE // head_dim)], axis=1)
                proj = jnp.dot(abuf[...], w, preferred_element_type=jnp.float32).astype(jnp.bfloat16)
                zrecv[c, :, cols] = (zrecv[c, :, cols].astype(jnp.float32) + proj.astype(jnp.float32)).astype(jnp.bfloat16)
                out_copy(c, k).start()
        hook(2)

    finish(6)
    with jax.named_scope('relay'):
        relay(0)
        relay(1)
        finish(7)
        relay(2)
    finish(8)
    plan = {(0, 2): (9,), (1, 2): (10, 11), (2, 0): (12,), (2, 1): (13,), (2, 2): (14, 15)}
    for c in range(n_tok):
        def hook(at, c=c):
            for j in plan.get((c, at), ()):
                with jax.named_scope('fin'):
                    if j == last:
                        finish_last()
                    else:
                        finish(j)
        with jax.named_scope('attend'):
            attend(c, hook)

    y_all.wait_send()
    z_all.wait_send()
    for d in range(n_col):
        d_copy(d).wait_send()
    for part in range(2):
        for r in range(3):
            t_copy(r, part).wait_send()
    pltpu.make_async_copy(zrecv, out_hbm, out_sem).wait()


def copy_kernel(src, dst, hold, in_sem, out_sem):
    steps = src.shape[0]
    for c in range(steps):
        pltpu.make_async_copy(src.at[c], hold.at[c], in_sem.at[c]).start()
    for c in range(steps):
        pltpu.make_async_copy(src.at[c], hold.at[c], in_sem.at[c]).wait()
        pltpu.make_async_copy(hold.at[c], dst.at[c], out_sem.at[c]).start()
    for c in range(steps):
        pltpu.make_async_copy(hold.at[c], dst.at[c], out_sem.at[c]).wait()


def settle(x):
    anyspace = pl.BlockSpec(memory_space=pl.ANY)
    dma = pltpu.SemaphoreType.DMA
    return pl.pallas_call(copy_kernel, out_shape=jax.ShapeDtypeStruct(x.shape, x.dtype), in_specs=[anyspace], out_specs=anyspace,
                          scratch_shapes=[pltpu.VMEM(x.shape, x.dtype), dma((x.shape[0],)), dma((x.shape[0],))])(x)


def run_stage(pp_size, heads, expert_out, ids, slot, gate, resid, scale, wq, wk, wv, wo):
    experts, cap_all, width = expert_out.shape
    tokens = resid.shape[0]
    slots = experts * cap_all // 4
    n_tok, n_col = tokens // TOK, width // COL
    n_piece = n_tok * n_col
    dma = pltpu.SemaphoreType.DMA
    anyspace = pl.BlockSpec(memory_space=pl.ANY)
    vmem = pl.BlockSpec(memory_space=pltpu.VMEM)
    f32, bf16 = jnp.float32, jnp.bfloat16
    return pl.pallas_call(
        functools.partial(stage_kernel, pp_size, heads),
        out_shape=jax.ShapeDtypeStruct((n_tok, TOK, width), bf16),
        in_specs=[anyspace, vmem, vmem, vmem, anyspace, vmem, anyspace, anyspace, anyspace, anyspace],
        out_specs=anyspace,
        scratch_shapes=[
            pltpu.VMEM((max(4 * slots, 3 * width), width), bf16),
            pltpu.VMEM((16, tokens), f32), pltpu.VMEM((3, 16, tokens), f32),
            pltpu.VMEM((tokens, 64), f32),
            pltpu.VMEM((3 * TOK, slots), bf16), pltpu.VMEM((3 * TOK, slots), bf16),
            pltpu.VMEM((n_piece, TOK, COL), f32), pltpu.VMEM((n_piece, TOK, COL), f32), pltpu.VMEM((n_piece, TOK, COL), f32),
            pltpu.VMEM((n_col, TOK, COL), f32), pltpu.VMEM((n_col, TOK, COL), f32),
            pltpu.VMEM((n_piece, TOK, COL), bf16),
            pltpu.VMEM((n_tok, TOK, width), bf16),
            pltpu.VMEM((width // BLK, width, width // heads), bf16),
            pltpu.VMEM((TOK, width), bf16), pltpu.VMEM((tokens, width), bf16), pltpu.VMEM((tokens, width), bf16), pltpu.VMEM((TOK, width), bf16), pltpu.VMEM((TOK, width), bf16),
            dma((4,)), dma((n_tok,)), dma((2, 3)), dma((2, 3)), dma((n_col,)), dma((n_col,)),
            pltpu.SemaphoreType.REGULAR,
            dma, dma((n_piece - 1,)), dma, dma((n_tok,)), dma((PARTS,)), dma((width // BLK,)), dma,
        ],
        compiler_params=pltpu.CompilerParams(collective_id=0, has_side_effects=True, vmem_limit_bytes=67043328),
    )(expert_out, ids, slot, gate, resid, scale, wq, wk, wv, wo)


def solution(mesh):
    pp_size = mesh.shape['pp']
    token_spec = P(('data', 'pp'), 'ep', None, None)
    weight_spec = P('pp', None, None, None)

    def body(expert_out, expert_ids, slot_ids, gate_vals, residual, norm_scale, w_query, w_key, w_value, w_out):
        ids, slot, gate = (jnp.swapaxes(a[0, 0], 0, 1) for a in (expert_ids, slot_ids, gate_vals))
        result = run_stage(pp_size, w_query.shape[2], expert_out[0], ids, slot, gate, residual[0, 0], norm_scale,
                           *(w[0].reshape(-1, w.shape[-1]) for w in (w_query, w_key, w_value, w_out)))
        return settle(result).reshape(residual.shape)

    return jax.shard_map(body, mesh=mesh, in_specs=(token_spec, token_spec, token_spec, token_spec, token_spec, P('pp', None), weight_spec, weight_spec, weight_spec, weight_spec), out_specs=token_spec, check_vma=False)
```

```python
import functools

import jax
import jax.numpy as jnp
from jax import lax
from jax.experimental import pallas as pl
from jax.experimental.pallas import tpu as pltpu
from jax.sharding import PartitionSpec as P

NORM_EPS = 1e-6
MESH = pl.DeviceIdType.MESH
TOK = 128
COL = 512
WIDE = 1024
BLK = 128
PARTS = 8


def stage_kernel(pp_size, heads, o_hbm, ids_hbm, slot_hbm, gate_hbm, h_hbm, scale_hbm, wq_hbm, wk_hbm, wv_hbm, wo_hbm, out_hbm,
                 ids_in, slot_in, gate_in, scale_in, i_sem, arena, mine, theirs, tblt, gate_a, gate_b, ysend, acc, yrecv, dsend, drecv, hz, zrecv, panel, qbuf, kbuf, vbuf, xbuf, abuf,
                 o_sem, h_sem, t_ssem, t_rsem, d_ssem, d_rsem, credit, y_ssem, y_rsem, z_ssem, z_rsem, yp_rsem, s_sem, out_sem):
    experts, cap_all, width = o_hbm.shape
    cap = cap_all // 4
    slots = experts * cap
    tokens = h_hbm.shape[0]
    head_dim = width // heads
    n_tok, n_col = tokens // TOK, width // COL
    n_piece = n_tok * n_col
    gates = (gate_b, gate_a)
    me = lax.axis_index('ep')
    core = lax.rem(me, 2)
    row = me // 2
    partner = row * 2 + (1 - core)
    peer = (1 - row) * 2 + core
    diag = (1 - row) * 2 + (1 - core)
    owners = (diag, peer, partner, me)
    stage = lax.axis_index('pp')
    nxt = lax.rem(stage + 1, pp_size)
    prv = lax.rem(stage + pp_size - 1, pp_size)

    def o_start(r):
        def one(e, _):
            pltpu.make_async_copy(o_hbm.at[e, pl.ds(owners[r] * cap, cap)],
                                  arena.at[pl.ds(pl.multiple_of(r * slots + e * cap, 16), cap)], o_sem.at[r]).start()
            return 0
        lax.fori_loop(0, experts, one, 0)

    def o_wait(r):
        view = arena.at[pl.ds(r * slots, slots)]
        pltpu.make_async_copy(view, view, o_sem.at[r]).wait()

    def h_copy(i):
        c, d = i // n_col, i % n_col
        return pltpu.make_async_copy(h_hbm.at[pl.ds(c * TOK, TOK), pl.ds(d * COL, COL)], hz.at[i], h_sem.at[c])

    cuts = (pl.ds(0, TOK), pl.ds(TOK, tokens - TOK))

    def t_copy(r, part):
        at = cuts[part]
        return pltpu.make_async_remote_copy(src_ref=mine.at[:, at], dst_ref=theirs.at[r, :, at], send_sem=t_ssem.at[part, r],
                                            recv_sem=t_rsem.at[part, r], device_id={'ep': owners[r]}, device_id_type=MESH)

    def d_copy(d):
        return pltpu.make_async_remote_copy(src_ref=dsend.at[d], dst_ref=drecv.at[d], send_sem=d_ssem.at[d],
                                            recv_sem=d_rsem.at[d], device_id={'ep': partner}, device_id_type=MESH)

    def y_copy(i):
        return pltpu.make_async_remote_copy(src_ref=ysend.at[i], dst_ref=yrecv.at[i], send_sem=y_ssem, recv_sem=y_rsem.at[i],
                                            device_id={'ep': peer}, device_id_type=MESH)

    def z_copy(i):
        c, d = i // n_col, i % n_col
        return pltpu.make_async_remote_copy(src_ref=hz.at[i], dst_ref=zrecv.at[c, :, pl.ds(pl.multiple_of(d * COL, COL), COL)],
                                            send_sem=z_ssem, recv_sem=z_rsem.at[c], device_id={'pp': nxt}, device_id_type=MESH)

    y_all = pltpu.make_async_remote_copy(src_ref=ysend, dst_ref=ysend, send_sem=y_ssem, recv_sem=y_rsem.at[0],
                                         device_id={'ep': peer}, device_id_type=MESH)
    z_all = pltpu.make_async_remote_copy(src_ref=hz, dst_ref=hz, send_sem=z_ssem, recv_sem=z_rsem.at[0],
                                         device_id={'pp': nxt}, device_id_type=MESH)
    last = n_piece - 1
    thin = TOK // PARTS

    def y_part(k):
        rows = pl.ds(k * thin, thin)
        return pltpu.make_async_remote_copy(src_ref=ysend.at[last, rows], dst_ref=yrecv.at[last, rows], send_sem=y_ssem,
                                            recv_sem=yp_rsem.at[k], device_id={'ep': peer}, device_id_type=MESH)

    def z_part(k):
        rows = pl.ds(k * thin, thin)
        return pltpu.make_async_remote_copy(src_ref=hz.at[last, rows], dst_ref=zrecv.at[n_tok - 1, rows, pl.ds(width - COL, COL)],
                                            send_sem=z_ssem, recv_sem=z_rsem.at[n_tok - 1], device_id={'pp': nxt}, device_id_type=MESH)

    raw = (wq_hbm, wk_hbm, wv_hbm)

    n_blk = width // BLK
    rows_blk = BLK * heads

    def s_copy(w, b):
        return pltpu.make_async_copy(raw[w].at[pl.ds(b * rows_blk, rows_blk)], panel.at[b], s_sem.at[b])

    def w_copy(q):
        return pltpu.make_async_copy(wo_hbm.at[:, pl.ds(q * head_dim, head_dim)], panel.at[q], s_sem.at[q])

    def keyed(r, table, part):
        lane_row = lax.broadcasted_iota(jnp.int32, table.shape, 0)
        shift = jnp.where(lane_row < 8, me * slots, 0).astype(jnp.float32)
        tblt[cuts[part], r * 16:(r + 1) * 16] = jnp.transpose(table - shift)

    groups = TOK // 16

    def build(c, r, q):
        t = tblt[pl.ds(pl.multiple_of(c * TOK + q * 16, 16), 16), r * 16:(r + 1) * 16]
        lane = lax.broadcasted_iota(jnp.int32, (16, slots), 1).astype(jnp.float32)
        g = jnp.zeros((16, slots), jnp.float32)
        for j in range(8):
            g = jnp.where(lane == t[:, j:j + 1], t[:, 8 + j:9 + j], g)
        g1 = g.astype(jnp.bfloat16)
        rest = g - g1.astype(jnp.float32)
        g2 = rest.astype(jnp.bfloat16)
        g3 = (rest - g2.astype(jnp.float32)).astype(jnp.bfloat16)
        at = pl.multiple_of(q * 16, 16)
        dst = gates[r % 2]
        dst[pl.ds(at, 16), :] = g1
        dst[pl.ds(at + TOK, 16), :] = g2
        dst[pl.ds(at + 2 * TOK, 16), :] = g3

    halves = width // WIDE

    def dot_role(r, h, per):
        w = arena[r * slots:(r + 1) * slots, h * COL:(h + per) * COL]
        p = jnp.dot(gates[r % 2][...], w, preferred_element_type=jnp.float32)
        total = p[:TOK] + p[TOK:2 * TOK] + p[2 * TOK:]
        return [(h + u, total[:, u * COL:(u + 1) * COL]) for u in range(per)]

    def build_now(c, r):
        for q in range(groups):
            build(c, r, q)

    def give():
        pl.semaphore_signal(credit, inc=1, device_id={'ep': partner}, device_id_type=MESH)

    def hold(d):
        d_copy(d).wait_send()
        pl.semaphore_wait(credit, 1)

    def finish(j):
        y_copy(j).wait_recv()
        hz[j] = (acc[j] + yrecv[j]).astype(jnp.bfloat16)
        z_copy(j).start()

    def finish_last():
        for k in range(PARTS):
            rows = pl.ds(k * thin, thin)
            y_part(k).wait_recv()
            hz[last, rows] = (acc[last, rows] + yrecv[last, rows]).astype(jnp.bfloat16)
            z_part(k).start()

    smalls = ((ids_hbm, ids_in), (slot_hbm, slot_in), (gate_hbm, gate_in), (scale_hbm, scale_in))

    def small(k):
        return pltpu.make_async_copy(*smalls[k], i_sem.at[k])

    barrier = pltpu.get_barrier_semaphore()
    for dev in (partner, peer, diag):
        pl.semaphore_signal(barrier, inc=1, device_id={'ep': dev}, device_id_type=MESH)
    for dev in (nxt, prv):
        pl.semaphore_signal(barrier, inc=1, device_id={'pp': dev}, device_id_type=MESH)
    for k in range(3):
        small(k).start()
    o_start(0)
    small(3).start()
    for k in range(3):
        small(k).wait()
    slot = slot_in[...]
    mine[0:8] = jnp.where(slot >= 0, ids_in[...] * cap + (slot - me * cap), -1).astype(jnp.float32)
    mine[8:16] = gate_in[...]
    pl.semaphore_wait(barrier, 5)
    for part in range(2):
        for r in range(3):
            t_copy(r, part).start()
    o_start(1)
    for part in range(2):
        keyed(3, mine[:, cuts[part]], part)

    def table(r, part):
        t_copy(r, part).wait_recv()
        keyed(r, theirs[r, :, cuts[part]], part)

    table(0, 0)
    build_now(0, 0)
    table(1, 0)

    def later():
        o_start(2)
        o_start(3)
        small(3).wait()

        def one(i, _):
            h_copy(i).start()
            return 0
        lax.fori_loop(0, n_piece, one, 0)
        table(2, 0)
        for r in range(3):
            table(r, 1)

    def at_first(c, r):
        @pl.when(c == 0)
        def _():
            o_wait(r)

    def chunk(c, _):
        @pl.when(c == 1)
        def _():
            for q in range(n_blk):
                s_copy(0, q).start()

        def fill(d):
            i = c * n_col + d
            d_copy(d).wait_recv()
            ysend[i] += drecv[d]
            give()
            if d < n_col - 1:
                y_copy(i).start()
            else:
                @pl.when(c < n_tok - 1)
                def _():
                    y_copy(i).start()

                @pl.when(c == n_tok - 1)
                def _():
                    for k in range(PARTS):
                        y_part(k).start()

        def out_role(r, h, per, ahead=None):
            for d in range(h, h + per):
                if r == 0:
                    @pl.when(c > 0)
                    def _():
                        hold(d)
                else:
                    hold(d)
            if h == 0:
                at_first(c, r)
            for d, value in dot_role(r, h, per):
                dsend[d] = value
            if ahead is not None:
                build_now(*ahead)
            for d in range(h, h + per):
                d_copy(d).start()

        def near_role(h, per, ahead=None):
            if h == 0:
                at_first(c, 1)
            for d, value in dot_role(1, h, per):
                ysend[c * n_col + d] = value
            if ahead is not None:
                build_now(*ahead)
            for d in range(h, h + per):
                fill(d)

        def own_role(h, per, ahead=None):
            if h == 0:
                view = hz.at[pl.ds(c * n_col, n_col)]
                pltpu.make_async_copy(view, view, h_sem.at[c]).wait()
                at_first(c, 3)
            for d, value in dot_role(3, h, per):
                i = c * n_col + d
                acc[i] = value + hz[i].astype(jnp.float32)
            if ahead is not None:
                build_now(*ahead)
            for d in range(h, h + per):
                d_copy(d).wait_recv()
                acc[c * n_col + d] += drecv[d]

                @pl.when(c < n_tok - 1)
                def _():
                    give()

        half = n_col // 2
        out_role(0, 0, 1, (c, 1))

        for d in range(1, half):
            out_role(0, d, 1)
        for d in range(half):
            near_role(d, 1)
            if d == 0:
                pl.when(c == 0)(later)
        out_role(0, half, half)
        near_role(half, half, (c, 2))
        out_role(2, 0, half, (c, 3))
        out_role(2, half, half)
        own_role(0, half)
        own_role(half, half, (lax.rem(c + 1, n_tok), 0))

        @pl.when(c > 0)
        def _():
            finish(2 * c - 2)
            finish(2 * c - 1)
        return 0

    with jax.named_scope('combine'):
        lax.fori_loop(0, n_tok, chunk, 0)

    def relay(w):
        def block(b, _):
            s_copy(w, b).wait()
            for k in range(BLK // 64):
                rows = panel[b, k * 64 * heads:(k + 1) * 64 * heads, :].reshape(64, heads, head_dim).reshape(64, width)
                arena[pl.ds(pl.multiple_of(w * width + b * BLK + k * 64, 64), 64), :] = rows
            if w < 2:
                s_copy(w + 1, b).start()
            else:
                w_copy(b).start()
            return 0
        lax.fori_loop(0, n_blk, block, 0)

    def out_copy(c, k):
        cols = pl.ds(k * WIDE, WIDE)
        return pltpu.make_async_copy(zrecv.at[c, :, cols], out_hbm.at[c, :, cols], out_sem)

    def attend(c, hook):
        with jax.named_scope('zwait'):
            pltpu.make_async_copy(zrecv.at[c], zrecv.at[c], z_rsem.at[c]).wait()
        scale = scale_in[...]
        for k in range(TOK // 16):
            rows = slice(k * 16, (k + 1) * 16)
            x = zrecv[c, rows, :].astype(jnp.float32)
            inv = lax.rsqrt(jnp.mean(x * x, axis=-1, keepdims=True) + NORM_EPS)
            xbuf[rows, :] = (x * inv * scale).astype(jnp.bfloat16)

        seen = (c + 1) * TOK
        q_at = lax.broadcasted_iota(jnp.int32, (TOK, seen), 0) + c * TOK
        k_at = lax.broadcasted_iota(jnp.int32, (TOK, seen), 1)
        causal = q_at >= k_at

        def project(n, wide):
            cols = pl.ds(n, wide)
            x = xbuf[...]
            qbuf[:, cols] = jnp.dot(x, arena[0:width, cols], preferred_element_type=jnp.float32).astype(jnp.bfloat16)
            kbuf[c * TOK:(c + 1) * TOK, cols] = jnp.dot(x, arena[width:2 * width, cols], preferred_element_type=jnp.float32).astype(jnp.bfloat16)
            vbuf[c * TOK:(c + 1) * TOK, cols] = jnp.dot(x, arena[2 * width:3 * width, cols], preferred_element_type=jnp.float32).astype(jnp.bfloat16)

        def mix(first, count):
            cols = [pl.ds((first + u) * head_dim, head_dim) for u in range(count)]
            logits = [lax.dot_general(qbuf[:, at], kbuf[0:seen, at], (((1,), (1,)), ((), ())), preferred_element_type=jnp.float32) for at in cols]
            logits = [jnp.where(causal, s * (head_dim ** -0.5), -1e30) for s in logits]
            probs = [jnp.exp(s - jnp.max(s, axis=-1, keepdims=True)) for s in logits]
            sums = [jnp.sum(p, axis=-1, keepdims=True) for p in probs]
            mixed = [jnp.dot(p.astype(jnp.bfloat16), vbuf[0:seen, at], preferred_element_type=jnp.float32) for p, at in zip(probs, cols)]
            for at, m, t in zip(cols, mixed, sums):
                abuf[:, at] = (m / t).astype(jnp.bfloat16)

        if c == n_tok - 1:
            with jax.named_scope('lastmix'):
                for k in range(halves):
                    project(k * WIDE, WIDE)
                    mix(k * heads // halves, heads // halves)
        else:
            def one(n, _):
                project(pl.multiple_of(n * WIDE, WIDE), WIDE)
                return 0
            with jax.named_scope('project'):
                lax.fori_loop(0, halves, one, 0)
            hook(0)
            with jax.named_scope('heads'):
                mix(0, heads)
            hook(1)
        if c == 0:
            for q in range(heads):
                w_copy(q).wait()
        with jax.named_scope('output'):
            for k in range(halves):
                cols = slice(k * WIDE, (k + 1) * WIDE)
                w = jnp.concatenate([panel[q] for q in range(k * WIDE // head_dim, (k + 1) * WIDE // head_dim)], axis=1)
                proj = jnp.dot(abuf[...], w, preferred_element_type=jnp.float32).astype(jnp.bfloat16)
                zrecv[c, :, cols] = (zrecv[c, :, cols].astype(jnp.float32) + proj.astype(jnp.float32)).astype(jnp.bfloat16)
                out_copy(c, k).start()
        hook(2)

    finish(6)
    with jax.named_scope('relay'):
        relay(0)
        relay(1)
        finish(7)
        relay(2)
    finish(8)
    plan = {(0, 2): (9,), (1, 2): (10, 11), (2, 0): (12,), (2, 1): (13,), (2, 2): (14, 15)}
    for c in range(n_tok):
        def hook(at, c=c):
            for j in plan.get((c, at), ()):
                with jax.named_scope('fin'):
                    if j == last:
                        finish_last()
                    else:
                        finish(j)
        with jax.named_scope('attend'):
            attend(c, hook)

    y_all.wait_send()
    z_all.wait_send()
    for d in range(n_col):
        d_copy(d).wait_send()
    for part in range(2):
        for r in range(3):
            t_copy(r, part).wait_send()
    pltpu.make_async_copy(zrecv, out_hbm, out_sem).wait()


def copy_kernel(src, dst, hold, in_sem, out_sem):
    steps = src.shape[0]
    for c in range(steps):
        pltpu.make_async_copy(src.at[c], hold.at[c], in_sem.at[c]).start()
    for c in range(steps):
        pltpu.make_async_copy(src.at[c], hold.at[c], in_sem.at[c]).wait()
        pltpu.make_async_copy(hold.at[c], dst.at[c], out_sem.at[c]).start()
    for c in range(steps):
        pltpu.make_async_copy(hold.at[c], dst.at[c], out_sem.at[c]).wait()


def settle(x):
    anyspace = pl.BlockSpec(memory_space=pl.ANY)
    dma = pltpu.SemaphoreType.DMA
    return pl.pallas_call(copy_kernel, out_shape=jax.ShapeDtypeStruct(x.shape, x.dtype), in_specs=[anyspace], out_specs=anyspace,
                          scratch_shapes=[pltpu.VMEM(x.shape, x.dtype), dma((x.shape[0],)), dma((x.shape[0],))])(x)


def run_stage(pp_size, heads, expert_out, ids, slot, gate, resid, scale, wq, wk, wv, wo):
    experts, cap_all, width = expert_out.shape
    tokens = resid.shape[0]
    slots = experts * cap_all // 4
    n_tok, n_col = tokens // TOK, width // COL
    n_piece = n_tok * n_col
    dma = pltpu.SemaphoreType.DMA
    anyspace = pl.BlockSpec(memory_space=pl.ANY)
    f32, bf16 = jnp.float32, jnp.bfloat16
    return pl.pallas_call(
        functools.partial(stage_kernel, pp_size, heads),
        out_shape=jax.ShapeDtypeStruct((n_tok, TOK, width), bf16),
        in_specs=[anyspace] * 10,
        out_specs=anyspace,
        scratch_shapes=[
            pltpu.VMEM(ids.shape, jnp.int32), pltpu.VMEM(slot.shape, jnp.int32), pltpu.VMEM(gate.shape, f32), pltpu.VMEM(scale.shape, f32), dma((4,)),
            pltpu.VMEM((max(4 * slots, 3 * width), width), bf16),
            pltpu.VMEM((16, tokens), f32), pltpu.VMEM((3, 16, tokens), f32),
            pltpu.VMEM((tokens, 64), f32),
            pltpu.VMEM((3 * TOK, slots), bf16), pltpu.VMEM((3 * TOK, slots), bf16),
            pltpu.VMEM((n_piece, TOK, COL), f32), pltpu.VMEM((n_piece, TOK, COL), f32), pltpu.VMEM((n_piece, TOK, COL), f32),
            pltpu.VMEM((n_col, TOK, COL), f32), pltpu.VMEM((n_col, TOK, COL), f32),
            pltpu.VMEM((n_piece, TOK, COL), bf16),
            pltpu.VMEM((n_tok, TOK, width), bf16),
            pltpu.VMEM((width // BLK, width, width // heads), bf16),
            pltpu.VMEM((TOK, width), bf16), pltpu.VMEM((tokens, width), bf16), pltpu.VMEM((tokens, width), bf16), pltpu.VMEM((TOK, width), bf16), pltpu.VMEM((TOK, width), bf16),
            dma((4,)), dma((n_tok,)), dma((2, 3)), dma((2, 3)), dma((n_col,)), dma((n_col,)),
            pltpu.SemaphoreType.REGULAR,
            dma, dma((n_piece - 1,)), dma, dma((n_tok,)), dma((PARTS,)), dma((width // BLK,)), dma,
        ],
        compiler_params=pltpu.CompilerParams(collective_id=0, has_side_effects=True, vmem_limit_bytes=67043328),
    )(expert_out, ids, slot, gate, resid, scale, wq, wk, wv, wo)


def solution(mesh):
    pp_size = mesh.shape['pp']
    token_spec = P(('data', 'pp'), 'ep', None, None)
    weight_spec = P('pp', None, None, None)

    def body(expert_out, expert_ids, slot_ids, gate_vals, residual, norm_scale, w_query, w_key, w_value, w_out):
        ids, slot, gate = (jnp.swapaxes(a[0, 0], 0, 1) for a in (expert_ids, slot_ids, gate_vals))
        result = run_stage(pp_size, w_query.shape[2], expert_out[0], ids, slot, gate, residual[0, 0], norm_scale,
                           *(w[0].reshape(-1, w.shape[-1]) for w in (w_query, w_key, w_value, w_out)))
        return settle(result).reshape(residual.shape)

    return jax.shard_map(body, mesh=mesh, in_specs=(token_spec, token_spec, token_spec, token_spec, token_spec, P('pp', None), weight_spec, weight_spec, weight_spec, weight_spec), out_specs=token_spec, check_vma=False)
```
